128 devices in a mesh: dp: 8 (over y, x_lo), tensor: 16 (over x_hi, z, core).
Axes of the slice: x: 4 (x_hi: 2, x_lo: 2; x = x_hi * 2 + x_lo), y: 4, z: 4, core: 2. Of those that a mesh axis runs over, the one named last changes fastest.
Arguments:
- grad_out: bfloat16 [8192, 8192], P(('dp', 'tensor')), may hold values from -24 to 24
- out_weight: bfloat16 [8192, 8192], P('dp', 'tensor'), may hold values from -0.0625 to 0.0625
- query: bfloat16 [8192, 8192], P('dp', 'tensor'), may hold values from -6 to 6, as said below
- keys: bfloat16 [8192, 512], P('dp'), may hold values from -6 to 6
- values: bfloat16 [8192, 512], P('dp'), may hold values from -6 to 6
- attended: bfloat16 [8192, 8192], P('dp', 'tensor'), may hold values from -6 to 6, as said below
- stats: float32 [64, 8192], P('tensor', 'dp'), as said below
Outputs:
- query_grad: bfloat16 [8192, 8192], P('dp', 'tensor')
- key_grad: bfloat16 [8192, 512], P('dp', 'tensor')
- value_grad: bfloat16 [8192, 512], P('dp', 'tensor')
- weight_grad: bfloat16 [8192, 8192], P('dp', 'tensor')
The draws below stay inside these ranges and needn't reach their ends.
Inputs may be any that keep to these rules, and one draw needn't show every extreme that they name: query, keys and values are independent draws. attended is the causal attention output of the given query, keys and values within each sequence of 1024 rows: query head h uses key head h // 16, scores scaled by 128 ** -0.5, softmax over keys at or before the query. stats[h, t] is the logarithm of the sum of exp(score) over the keys that row t of head h attends to, for the same scores.
All inputs are finite; a program needn't handle non-finite values.
Results may differ from the reference program's by a relative error of at most 0.013.
Values may be sent and summed in bfloat16 or wider, within the bound.
A program may use at most 192 MiB of HBM per device.

```python
import jax
import jax.numpy as jnp
from jax import lax

D = 8192
HD = 128
GROUP = 16
LEN = 1024
HEADS = 64
KV_HEADS = 4
TOKENS = 8192


def draw_inputs(key):
    key_query = jax.random.fold_in(key, 101)
    key_keys = jax.random.fold_in(key, 202)
    key_values = jax.random.fold_in(key, 303)
    query = jnp.clip(jax.random.normal(key_query, (TOKENS, HEADS * HD), jnp.float32), -6.0, 6.0)
    keys = jnp.clip(jax.random.normal(key_keys, (TOKENS, KV_HEADS * HD), jnp.float32), -6.0, 6.0)
    values = jnp.clip(jax.random.normal(key_values, (TOKENS, KV_HEADS * HD), jnp.float32), -6.0, 6.0)
    return (query.astype(jnp.bfloat16), keys.astype(jnp.bfloat16), values.astype(jnp.bfloat16))


def forward_pass(key):
    query, keys, values = draw_inputs(key)
    seq_count = TOKENS // LEN
    query_split = query.astype(jnp.float32).reshape(seq_count, LEN, KV_HEADS, GROUP, HD)
    query_split = query_split.transpose(0, 2, 3, 1, 4).reshape(seq_count * KV_HEADS, GROUP, LEN, HD)
    keys_split = keys.astype(jnp.float32).reshape(seq_count, LEN, KV_HEADS, HD)
    keys_split = keys_split.transpose(0, 2, 1, 3).reshape(seq_count * KV_HEADS, LEN, HD)
    values_split = values.astype(jnp.float32).reshape(seq_count, LEN, KV_HEADS, HD)
    values_split = values_split.transpose(0, 2, 1, 3).reshape(seq_count * KV_HEADS, LEN, HD)
    positions = jnp.arange(LEN, dtype=jnp.int32)
    causal = positions[:, None] >= positions[None, :]

    def single(inputs):
        query_group, key_one, value_one = inputs
        scores = jnp.einsum('gqd,kd->gqk', query_group, key_one) * HD ** (-0.5)
        masked = jnp.where(causal[None], scores, -1e+30)
        highest = jnp.max(masked, axis=2, keepdims=True)
        log_total = highest[:, :, 0] + jnp.log(jnp.sum(jnp.exp(masked - highest), axis=2))
        weights_soft = jnp.exp(masked - log_total[:, :, None])
        output = jnp.einsum('gqk,kd->gqd', weights_soft, value_one)
        return (output, log_total)
    outputs, log_totals = lax.map(single, (query_split, keys_split, values_split))
    attended = outputs.reshape(seq_count, KV_HEADS, GROUP, LEN, HD).transpose(0, 3, 1, 2, 4)
    attended = attended.reshape(TOKENS, HEADS * HD)
    stats = log_totals.reshape(seq_count, KV_HEADS, GROUP, LEN).transpose(1, 2, 0, 3).reshape(HEADS, TOKENS)
    return (attended, stats)


def draw_query(key, part):
    return draw_inputs(key)[0]


def draw_keys(key, part):
    return draw_inputs(key)[1]


def draw_values(key, part):
    return draw_inputs(key)[2]


def draw_attended(key, part):
    return forward_pass(key)[0].astype(jnp.bfloat16)


def draw_stats(key, part):
    return forward_pass(key)[1].astype(jnp.float32)


def spiked(drawn, rng, source, target, shards_of, factor):
    owner, partner = [(jnp.arange(drawn.shape[dim]) // (drawn.shape[dim] // shards_of)).reshape([-1 if axis == dim else 1 for axis in range(drawn.ndim)]) for dim in (source, target)]
    chosen = jax.random.permutation(rng, shards_of)[partner]
    strong = (owner == chosen) | (owner == (partner + shards_of // 2) % shards_of)
    return jnp.where(strong, factor * drawn, drawn)


def block_levels(rng, dims, split, low, high):
    factor_of = 1.0
    for dim, blocks in split:
        heights = jax.random.uniform(jax.random.fold_in(jax.random.fold_in(rng, 6), dim), (blocks,), jnp.float32, low / len(split), high / len(split))
        factor_of = factor_of * jnp.repeat(jnp.exp(heights), dims[dim] // blocks).reshape((-1,) + (1,) * (len(dims) - 1 - dim))
    return factor_of


def noise(rng, dims, width, reach, cuts=(), kind=jnp.bfloat16):
    loudness = block_levels(rng, dims, cuts, -0.22, 0.18) if cuts else 1.0
    entries = jax.random.normal(rng, dims, jnp.float32) * width * loudness
    return jnp.minimum(jnp.maximum(entries, -reach), reach).astype(kind)


def gaussian_with(own_key, extent, deviation, reach, cuts, heavy, kind=jnp.bfloat16):
    entries = deviation * jax.random.normal(own_key, extent, jnp.float32)
    if cuts:
        entries = entries * block_levels(own_key, extent, cuts, -0.22, 0.18)
    return jnp.clip(spiked(entries, jax.random.fold_in(own_key, 3), *heavy), -reach, reach).astype(kind)


def setup_inputs(seed: int = 0) -> dict:
    key_of = jax.random.split(jax.random.key(seed), 8)
    return {
        "grad_out": gaussian_with(key_of[0], (TOKENS, D), 1.0, 24.0, ((0, 128),), (0, 1, 128, 5.5)),
        "out_weight": noise(key_of[1], (D, HEADS * HD), D ** -0.5, 0.0625, ((0, 8), (1, 16))),
        "query": draw_query(jax.random.fold_in(key_of[7], 71), 0),
        "keys": draw_keys(jax.random.fold_in(key_of[7], 71), 0),
        "values": draw_values(jax.random.fold_in(key_of[7], 71), 0),
        "attended": draw_attended(jax.random.fold_in(key_of[7], 71), 0),
        "stats": draw_stats(jax.random.fold_in(key_of[7], 71), 0),
    }


def split_heads(array, seq_count):
    shaped = array.reshape(seq_count, LEN, KV_HEADS, GROUP, HD).transpose(0, 2, 3, 1, 4)
    return shaped.reshape(seq_count * KV_HEADS, GROUP, LEN, HD)

def join_heads(array, seq_count):
    shaped = array.reshape(seq_count, KV_HEADS, GROUP, LEN, HD).transpose(0, 3, 1, 2, 4)
    return shaped.reshape(seq_count * LEN, KV_HEADS * GROUP * HD)

def split_keys(array, seq_count):
    shaped = array.reshape(seq_count, LEN, KV_HEADS, HD).transpose(0, 2, 1, 3)
    return shaped.reshape(seq_count * KV_HEADS, LEN, HD)

def join_keys(array, seq_count):
    shaped = array.reshape(seq_count, KV_HEADS, LEN, HD).transpose(0, 2, 1, 3)
    return shaped.reshape(seq_count * LEN, KV_HEADS * HD)

def head_grads(inputs):
    query_group, key_one, value_one, attended_group, grad_group, stats_group = inputs
    score_scale = HD ** (-0.5)
    query_wide = query_group.astype(jnp.float32)
    key_wide = key_one.astype(jnp.float32)
    grad_wide = grad_group.astype(jnp.float32)
    positions = jnp.arange(LEN, dtype=jnp.int32)
    causal = positions[:, None] >= positions[None, :]
    scores = jnp.einsum('gqd,kd->gqk', query_wide, key_wide) * score_scale
    attention = jnp.where(causal[None], jnp.exp(scores - stats_group[:, :, None]), 0.0)
    attention_low = lax.optimization_barrier(attention.astype(jnp.bfloat16)).astype(jnp.float32)
    grad_attention = jnp.einsum('gqd,kd->gqk', grad_wide, value_one.astype(jnp.float32))
    row_offset = lax.optimization_barrier(jnp.sum(grad_wide * attended_group.astype(jnp.float32), axis=2))
    grad_scores = attention * (grad_attention - row_offset[:, :, None])
    grad_scores = lax.optimization_barrier(grad_scores.astype(jnp.bfloat16)).astype(jnp.float32)
    query_grad = (jnp.einsum('gqk,kd->gqd', grad_scores, key_wide) * score_scale).astype(jnp.bfloat16)
    key_grad = (jnp.einsum('gqk,gqd->kd', grad_scores, query_wide) * score_scale).astype(jnp.bfloat16)
    value_grad = jnp.einsum('gqk,gqd->kd', attention_low, grad_wide).astype(jnp.bfloat16)
    return (query_grad, key_grad, value_grad)

def reference(grad_out, out_weight, query, keys, values, attended, stats):
    seq_count = TOKENS // LEN
    grad_att = jnp.dot(grad_out, out_weight, preferred_element_type=jnp.float32).astype(jnp.bfloat16)
    grad_seqs = grad_out.reshape(seq_count, LEN, D)
    attended_seqs = attended.reshape(seq_count, LEN, HEADS * HD)

    def add_grad(running, pair):
        grad_block, attended_block = pair
        grad_term = lax.dot_general(grad_block, attended_block, (((0,), (0,)), ((), ())), preferred_element_type=jnp.float32)
        rounded = lax.optimization_barrier(grad_term.astype(jnp.bfloat16))
        return (running + rounded.astype(jnp.float32), None)
    weight_sum, _ = lax.scan(add_grad, jnp.zeros((D, HEADS * HD), jnp.float32), (grad_seqs, attended_seqs))
    weight_grad = weight_sum.astype(jnp.bfloat16)
    stats_split = stats.reshape(KV_HEADS, GROUP, seq_count, LEN).transpose(2, 0, 1, 3)
    stats_split = stats_split.reshape(seq_count * KV_HEADS, GROUP, LEN)
    query_parts, key_parts, value_parts = lax.map(head_grads, (split_heads(query, seq_count), split_keys(keys, seq_count), split_keys(values, seq_count), split_heads(attended, seq_count), split_heads(grad_att, seq_count), stats_split))
    query_grad = join_heads(query_parts, seq_count)
    key_grad = join_keys(key_parts, seq_count)
    value_grad = join_keys(value_parts, seq_count)
    return (query_grad, key_grad, value_grad, weight_grad)
```

```python
import jax
import jax.numpy as jnp
from jax import lax
from jax.experimental import pallas as pl
from jax.experimental.pallas import tpu as pltpu
from jax.sharding import Mesh
from jax.sharding import PartitionSpec as P

HD = 128
GROUP = 16
BF = jnp.bfloat16
F32 = jnp.float32
AXES = ("y", "xlo", "xhi", "z", "core")
NN = (((1,), (0,)), ((), ()))
NT = (((1,), (1,)), ((), ()))


def dot(a, b, dims=NN):
    return lax.dot_general(a, b, dims, preferred_element_type=F32)


def rcopy(src, dst, send, recv, dev):
    return pltpu.make_async_remote_copy(
        src_ref=src,
        dst_ref=dst,
        send_sem=send,
        recv_sem=recv,
        device_id=dev,
        device_id_type=pl.DeviceIdType.MESH,
    )


def kernel(
    g_in, w_in, q_in, k_in, v_in, a_in, st_in,
    dq_out, kv_out, wg_out,
    G, W, S, RX, RH, RP, RY, AT, ACC, Q, GA, GAT, K, V, KT, A, ST,
    DK, DV, KF, KB, KR1, KB2, KR2,
    xs, xr, us, ur, zs, zr, cs, cr, ws, wr, rs, rr, ks, kr, ls, lq,
):
    y, xlo, xhi = lax.axis_index("y"), lax.axis_index("xlo"), lax.axis_index("xhi")
    z, c = lax.axis_index("z"), lax.axis_index("core")
    scale = HD ** (-0.5)
    yp, ym, y2 = lax.rem(y + 1, 4), lax.rem(y + 3, 4), lax.rem(y + 2, 4)
    zp, zm, z2 = lax.rem(z + 1, 4), lax.rem(z + 3, 4), lax.rem(z + 2, 4)
    xo, xh, co = 1 - xlo, 1 - xhi, 1 - c
    zpair = z + 1 - 2 * lax.rem(z, 2)

    head = xhi * 2 + z // 2
    hcol = pl.ds(pl.multiple_of(head * HD, HD), HD)
    order = ((y2, xo), (y2, xlo), (yp, xo), (ym, xo), (yp, xlo), (ym, xlo), (y, xo), (y, xlo))

    own = []
    for j, (yj, xj) in enumerate(order):
        col = pl.multiple_of((yj * 2 + xj) * 1024, 1024)
        own.append(pltpu.make_async_copy(g_in.at[:, pl.ds(col, 1024)], G.at[j, xhi, z, c], ls.at[j]))
    for cp in own:
        cp.start()
    wcp = pltpu.make_async_copy(w_in, W.at[0], lq.at[0])
    wcp.start()
    acp = pltpu.make_async_copy(a_in, A, lq.at[1])
    acp.start()
    others = [
        pltpu.make_async_copy(k_in.at[:, hcol], K, lq.at[2]),
        pltpu.make_async_copy(v_in.at[:, hcol], V, lq.at[3]),
        pltpu.make_async_copy(st_in, ST, lq.at[4]),
    ]
    for h in range(4):
        others.append(
            pltpu.make_async_copy(q_in.at[:, h * HD : (h + 1) * HD], Q.at[h], lq.at[5 + h])
        )
    for cp in others:
        cp.start()

    barrier = pltpu.get_barrier_semaphore()
    for dev in ({"y": yp}, {"y": ym}, {"xlo": xo}, {"xhi": xh}, {"z": zp}, {"z": zm}, {"core": co}):
        pl.semaphore_signal(barrier, inc=1, device_id=dev, device_id_type=pl.DeviceIdType.MESH)
    pl.semaphore_wait(barrier, 7)

    def x_send(j):
        return rcopy(G.at[j, xhi, z, c], G.at[j, xhi, z, c], xs.at[j], xr.at[j], {"xhi": xh})

    def x_recv(j):
        return rcopy(G.at[j, xh, z, c], G.at[j, xh, z, c], xs.at[j], xr.at[j], {"xhi": xh})

    def unit(j, zz, cc):
        return G.at[j, :, zz, cc]

    def u_send(j, d):
        return rcopy(unit(j, z, c), unit(j, z, c), us.at[j, d], ur.at[j, d], {"z": (zp, zm)[d]})

    def u_recv(j, d):
        at = unit(j, (zm, zp)[d], c)
        return rcopy(at, at, us.at[j, d], ur.at[j, d], {"z": (zp, zm)[d]})

    def z_send(j, d):
        at = G.at[j, d, (zm, zp)[d], c]
        return rcopy(at, at, zs.at[j, d], zr.at[j, d], {"z": (zp, zm)[d]})

    def z_recv(j, d):
        at = G.at[j, d, z2, c]
        return rcopy(at, at, zs.at[j, d], zr.at[j, d], {"z": (zp, zm)[d]})

    slots = (z, zm, zp, z2)

    def c_send(j, s):
        at = unit(j, slots[s], c)
        return rcopy(at, at, cs.at[j, s], cr.at[j, s], {"core": co})

    def c_recv(j, s):
        at = unit(j, slots[s], co)
        return rcopy(at, at, cs.at[j, s], cr.at[j, s], {"core": co})

    top, low = pl.ds(0, 512), pl.ds(512, 512)
    wspec = (
        (W.at[0], W.at[2], {"y": yp}),
        (W.at[0], W.at[3], {"y": ym}),
        (W.at[0], W.at[1], {"xlo": xo}),
        (W.at[2, top], W.at[6, top], {"y": yp}),
        (W.at[3, low], W.at[6, low], {"y": ym}),
        (W.at[1], W.at[4], {"y": yp}),
        (W.at[1], W.at[5], {"y": ym}),
        (W.at[6], W.at[7], {"xlo": xo}),
    )

    def w_send(n):
        src, dst, dev = wspec[n]
        return rcopy(src, dst, ws.at[n], wr.at[n], dev)

    up, dn = pl.ds(0, 256), pl.ds(256, 256)
    rspec = (
        (S.at[0], RX.at[0], {"xlo": xo}),
        (S.at[1, up], RH.at[0], {"y": yp}),
        (S.at[1, dn], RH.at[1], {"y": ym}),
        (S.at[2], RP.at[0], {"y": yp}),
        (S.at[3], RP.at[1], {"y": ym}),
        (S.at[4], RY.at[0], {"y": yp}),
        (S.at[5], RY.at[1], {"y": ym}),
        (S.at[6], RX.at[1], {"xlo": xo}),
    )

    def r_send(n):
        src, dst, dev = rspec[n]
        return rcopy(src, dst, rs.at[n], rr.at[n], dev)

    def add_into(dst, rows, srcs):
        @pl.loop(0, rows // 64)
        def _(n):
            at = pl.ds(pl.multiple_of(n * 64, 64), 64)
            total = dst[at].astype(F32)
            for src in srcs:
                total = total + src[at].astype(F32)
            dst[at] = total.astype(BF)

    def weight_part(j):
        @pl.loop(0, 4)
        def _(n):
            at = pl.ds(pl.multiple_of(n * 256, 256), 256)
            rows = G[j, :, :, :, :, at].reshape(1024, 256)
            S[j, :, at] = dot(AT[...], rows).astype(BF)

    def att_part(j):
        @pl.loop(0, 2)
        def _(a):
            @pl.loop(0, 2)
            def _(b):
                at = pl.ds(pl.multiple_of((a * 2 + b) * 256, 256), 256)
                rows = G[j, a, pl.ds(b * 2, 2)].reshape(256, 1024)
                ACC[at] += dot(rows, W[7 - j])

    for j in range(8):
        own[j].wait()
        x_send(j).start()
    wcp.wait()
    for n in range(3):
        w_send(n).start()
    acp.wait()
    for h in range(4):
        AT[h * HD : (h + 1) * HD] = A[:, h * HD : (h + 1) * HD].T
    for cp in others:
        cp.wait()
    KT[...] = K[...].T
    ACC[...] = jnp.zeros_like(ACC)
    DK[...] = jnp.zeros_like(DK)
    DV[...] = jnp.zeros_like(DV)

    @pl.loop(0, 11)
    def _(i):
        @pl.when(i < 8)
        def _():
            x_recv(i).wait_recv()
            u_send(i, 0).start()
            u_send(i, 1).start()
            c_send(i, 0).start()

        @pl.when((i >= 1) & (i < 9))
        def _():
            j = i - 1
            for d in range(2):
                u_recv(j, d).wait_recv()
                z_send(j, d).start()
            c_send(j, 1).start()
            c_send(j, 2).start()

        @pl.when((i >= 2) & (i < 10))
        def _():
            j = i - 2
            for d in range(2):
                z_recv(j, d).wait_recv()
            c_send(j, 3).start()

        @pl.when(i >= 3)
        def _():
            j = i - 3
            for s in range(4):
                c_recv(j, s).wait_recv()
            weight_part(j)

        @pl.when(i == 3)
        def _():
            r_send(0).start()
            for n in range(3):
                w_send(n).wait_recv()
            for n in range(3, 7):
                w_send(n).start()

        @pl.when(i == 6)
        def _():
            for n in (3, 4):
                w_send(n).wait_recv()
            w_send(7).start()
            r_send(0).wait_recv()
            add_into(S.at[1], 512, [RX.at[0]])
            for n in range(1, 5):
                r_send(n).start()

        @pl.when(i >= 7)
        def _():
            att_part(i - 3)

    r_send(1).wait_recv()
    add_into(S.at[4, up], 256, [RH.at[0]])
    r_send(5).start()
    r_send(2).wait_recv()
    add_into(S.at[5, dn], 256, [RH.at[1]])
    r_send(6).start()

    w_send(5).wait_recv()
    w_send(6).wait_recv()

    @pl.loop(0, 4)
    def _(n):
        @pl.when(n == 3)
        def _():
            w_send(7).wait_recv()

        att_part(3 - n)

    for h in range(4):
        part = ACC[:, h * HD : (h + 1) * HD].astype(BF)
        GA[h] = part
        GAT[h] = part.T

    def r_mid():
        r_send(3).wait_recv()
        r_send(4).wait_recv()
        add_into(S.at[6], 512, [RP.at[0], RP.at[1]])
        r_send(7).start()

    @pl.loop(0, 4)
    def _(h):
        @pl.when(h == 2)
        def _():
            r_mid()

        for b in range(4):
            n = (b + 1) * 256
            lo = b * 256
            qb = Q[h, lo:n]
            gb = GA[h, lo:n]
            gt = GAT[h, :, lo:n]
            at_rows = AT[pl.ds(pl.multiple_of(h * HD, HD), HD), lo:n]
            offset = jnp.sum(gt.astype(F32) * at_rows.astype(F32), axis=0, keepdims=True)
            stat = ST[pl.ds(h, 1), lo:n]
            scores = dot(K[:n], qb, NT) * scale
            keys_at = lax.broadcasted_iota(jnp.int32, (n, 256), 0)
            query_at = lax.broadcasted_iota(jnp.int32, (n, 256), 1) + lo
            attention = jnp.where(keys_at <= query_at, jnp.exp(scores - stat), 0.0)
            DV[:n] += dot(attention.astype(BF), gb)
            grad_att = dot(V[:n], gb, NT)
            grad_scores = (attention * (grad_att - offset)).astype(BF)
            DK[:n] += dot(grad_scores, qb)
            dq = dot(KT[:, :n], grad_scores) * scale
            dq_out[lo:n, pl.ds(pl.multiple_of(h * HD, HD), HD)] = dq.T.astype(BF)

    zh = lax.rem(z, 2)
    dkt = (DK[...] * scale).T
    dvt = DV[...].T
    for n, full in enumerate((dkt, dvt)):
        for half in range(2):
            piece = full[half * 64 : half * 64 + 64]
            KF[n, half] = piece
            KB[half, n] = piece.astype(BF)
    k_send1 = rcopy(KB.at[1 - zh], KR1, ks.at[0], kr.at[0], {"z": zpair})
    k_send1.start()
    k_send1.wait_recv()
    for n in range(2):
        kept = KF[n, zh] + KR1[n].astype(F32)
        KF[n, 0] = kept
        KB2[0, n] = kept[:32].astype(BF)
        KB2[1, n] = kept[32:].astype(BF)
    k_send2 = rcopy(KB2.at[1 - c], KR2, ks.at[1], kr.at[1], {"core": co})
    k_send2.start()
    k_send2.wait_recv()
    for n in range(2):
        kv_out[n] = (KF[n, 0, pl.ds(pl.multiple_of(c * 32, 32), 32)] + KR2[n].astype(F32)).astype(BF)

    for n in (5, 6, 7):
        r_send(n).wait_recv()

    @pl.loop(0, 8)
    def _(n):
        at = pl.ds(pl.multiple_of(n * 64, 64), 64)
        total = S[7, at].astype(F32)
        for src in (RY.at[0], RY.at[1], RX.at[1]):
            total = total + src[at].astype(F32)
        wg_out[at] = total.astype(BF)

    @pl.loop(0, 8)
    def _(j):
        x_send(j).wait_send()
        for d in range(2):
            u_send(j, d).wait_send()
            z_send(j, d).wait_send()
        for s in range(4):
            c_send(j, s).wait_send()

    for n in range(8):
        w_send(n).wait_send()
        r_send(n).wait_send()
    k_send1.wait_send()
    k_send2.wait_send()


def per_device(grad_out, out_weight, query, keys, values, attended, stats):
    any_spec = pl.BlockSpec(memory_space=pl.ANY)
    vmem = pl.BlockSpec(memory_space=pltpu.VMEM)
    V_ = pltpu.VMEM
    dma = pltpu.SemaphoreType.DMA
    scratch = [
        V_((8, 2, 4, 2, 64, 1024), BF),
        V_((8, 1024, 512), BF),
        V_((8, 512, 1024), BF),
        V_((2, 512, 1024), BF),
        V_((2, 256, 1024), BF),
        V_((2, 512, 1024), BF),
        V_((2, 512, 1024), BF),
        V_((512, 1024), BF),
        V_((1024, 512), F32),
        V_((4, 1024, HD), BF),
        V_((4, 1024, HD), BF),
        V_((4, HD, 1024), BF),
        V_((1024, HD), BF),
        V_((1024, HD), BF),
        V_((HD, 1024), BF),
        V_((1024, 512), BF),
        V_((4, 1024), F32),
        V_((1024, HD), F32),
        V_((1024, HD), F32),
        V_((2, 2, 64, 1024), F32),
        V_((2, 2, 64, 1024), BF),
        V_((2, 64, 1024), BF),
        V_((2, 2, 32, 1024), BF),
        V_((2, 32, 1024), BF),
        dma((8,)), dma((8,)),
        dma((8, 2)), dma((8, 2)),
        dma((8, 2)), dma((8, 2)),
        dma((8, 4)), dma((8, 4)),
        dma((8,)), dma((8,)),
        dma((8,)), dma((8,)),
        dma((2,)), dma((2,)),
        dma((8,)), dma((9,)),
    ]
    dq, kv, wg = pl.pallas_call(
        kernel,
        out_shape=(
            jax.ShapeDtypeStruct((1024, 512), BF),
            jax.ShapeDtypeStruct((2, 32, 1024), BF),
            jax.ShapeDtypeStruct((512, 1024), BF),
        ),
        in_specs=[any_spec] * 7,
        out_specs=(vmem, vmem, vmem),
        scratch_shapes=scratch,
        compiler_params=pltpu.CompilerParams(
            collective_id=0, has_side_effects=True, vmem_limit_bytes=67_000_000
        ),
    )(grad_out, out_weight, query, keys, values, attended, stats)
    return (dq, kv[0].T, kv[1].T, wg.T)


def solution(mesh):
    torus = Mesh(mesh.devices.reshape(4, 2, 2, 4, 2), AXES)
    dp, tp = ("y", "xlo"), ("xhi", "z", "core")
    in_specs = (
        P(dp + tp, None),
        P(dp, tp),
        P(dp, tp),
        P(dp, None),
        P(dp, None),
        P(dp, tp),
        P(tp, dp),
    )
    out_specs = (P(dp, tp), P(dp, tp), P(dp, tp), P(dp, tp))
    return jax.shard_map(
        per_device, mesh=torus, in_specs=in_specs, out_specs=out_specs, check_vma=False
    )
```

```python
import jax
import jax.numpy as jnp
from jax import lax
from jax.experimental import pallas as pl
from jax.experimental.pallas import tpu as pltpu
from jax.sharding import Mesh
from jax.sharding import PartitionSpec as P

HD = 128
GROUP = 16
BF = jnp.bfloat16
F32 = jnp.float32
AXES = ("y", "xlo", "xhi", "z", "core")
NN = (((1,), (0,)), ((), ()))
NT = (((1,), (1,)), ((), ()))


def dot(a, b, dims=NN):
    return lax.dot_general(a, b, dims, preferred_element_type=F32)


def rcopy(src, dst, send, recv, dev):
    return pltpu.make_async_remote_copy(
        src_ref=src,
        dst_ref=dst,
        send_sem=send,
        recv_sem=recv,
        device_id=dev,
        device_id_type=pl.DeviceIdType.MESH,
    )


def kernel(
    g_in, w_in, q_in, k_in, v_in, a_in, st_in,
    dq_out, kv_out, wg_out,
    G, W, S, RX, RH, RP, RY, AT, ACC, Q, GA, GAT, K, V, KT, A, ST,
    P0, P1, P2, P3, DK, DV, KF, KB, KR1, KB2, KR2,
    xs, xr, us, ur, zs, zr, cs, cr, ws, wr, rs, rr, ks, kr, ls, lq,
):
    y, xlo, xhi = lax.axis_index("y"), lax.axis_index("xlo"), lax.axis_index("xhi")
    z, c = lax.axis_index("z"), lax.axis_index("core")
    scale = HD ** (-0.5)
    PT = (P0, P1, P2, P3)
    yp, ym, y2 = lax.rem(y + 1, 4), lax.rem(y + 3, 4), lax.rem(y + 2, 4)
    zp, zm, z2 = lax.rem(z + 1, 4), lax.rem(z + 3, 4), lax.rem(z + 2, 4)
    xo, xh, co = 1 - xlo, 1 - xhi, 1 - c
    zpair = z + 1 - 2 * lax.rem(z, 2)

    head = xhi * 2 + z // 2
    hcol = pl.ds(pl.multiple_of(head * HD, HD), HD)
    order = ((y2, xo), (y2, xlo), (yp, xo), (ym, xo), (yp, xlo), (ym, xlo), (y, xo), (y, xlo))

    own = []
    for j, (yj, xj) in enumerate(order):
        col = pl.multiple_of((yj * 2 + xj) * 1024, 1024)
        own.append(pltpu.make_async_copy(g_in.at[:, pl.ds(col, 1024)], G.at[j, xhi, z, c], ls.at[j]))
    for cp in own:
        cp.start()
    wcp = pltpu.make_async_copy(w_in, W.at[0], lq.at[0])
    wcp.start()
    acp = pltpu.make_async_copy(a_in, A, lq.at[1])
    acp.start()
    others = [
        pltpu.make_async_copy(k_in.at[:, hcol], K, lq.at[2]),
        pltpu.make_async_copy(v_in.at[:, hcol], V, lq.at[3]),
        pltpu.make_async_copy(st_in, ST, lq.at[4]),
    ]
    for h in range(4):
        others.append(
            pltpu.make_async_copy(q_in.at[:, h * HD : (h + 1) * HD], Q.at[h], lq.at[5 + h])
        )
    for cp in others:
        cp.start()

    barrier = pltpu.get_barrier_semaphore()
    for dev in ({"y": yp}, {"y": ym}, {"xlo": xo}, {"xhi": xh}, {"z": zp}, {"z": zm}, {"core": co}):
        pl.semaphore_signal(barrier, inc=1, device_id=dev, device_id_type=pl.DeviceIdType.MESH)
    pl.semaphore_wait(barrier, 7)

    def x_send(j):
        return rcopy(G.at[j, xhi, z, c], G.at[j, xhi, z, c], xs.at[j], xr.at[j], {"xhi": xh})

    def x_recv(j):
        return rcopy(G.at[j, xh, z, c], G.at[j, xh, z, c], xs.at[j], xr.at[j], {"xhi": xh})

    def unit(j, zz, cc):
        return G.at[j, :, zz, cc]

    def u_send(j, d, p):
        at = G.at[j, (xhi, xh)[p], z, c]
        return rcopy(at, at, us.at[j, d, p], ur.at[j, d, p], {"z": (zp, zm)[d]})

    def u_recv(j, d, p):
        at = G.at[j, (xhi, xh)[p], (zm, zp)[d], c]
        return rcopy(at, at, us.at[j, d, p], ur.at[j, d, p], {"z": (zp, zm)[d]})

    def z_send(j, d):
        at = G.at[j, d, (zm, zp)[d], c]
        return rcopy(at, at, zs.at[j, d], zr.at[j, d], {"z": (zp, zm)[d]})

    def z_recv(j, d):
        at = G.at[j, d, z2, c]
        return rcopy(at, at, zs.at[j, d], zr.at[j, d], {"z": (zp, zm)[d]})

    slots = (z, zm, zp, z2)

    def c_send(j, s):
        at = unit(j, slots[s], c)
        return rcopy(at, at, cs.at[j, s], cr.at[j, s], {"core": co})

    def c_recv(j, s):
        at = unit(j, slots[s], co)
        return rcopy(at, at, cs.at[j, s], cr.at[j, s], {"core": co})

    top, low = pl.ds(0, 512), pl.ds(512, 512)
    wspec = (
        (W.at[0, top], W.at[2, top], {"y": yp}),
        (W.at[0, low], W.at[3, low], {"y": ym}),
        (W.at[0, low], W.at[2, low], {"y": yp}),
        (W.at[0, top], W.at[3, top], {"y": ym}),
        (W.at[0, top], W.at[1, top], {"xlo": xo}),
        (W.at[0, low], W.at[1, low], {"xlo": xo}),
        (W.at[2, top], W.at[6, top], {"y": yp}),
        (W.at[3, low], W.at[6, low], {"y": ym}),
        (W.at[1, top], W.at[4, top], {"y": yp}),
        (W.at[1, top], W.at[5, top], {"y": ym}),
        (W.at[1, low], W.at[4, low], {"y": yp}),
        (W.at[1, low], W.at[5, low], {"y": ym}),
        (W.at[6, top], W.at[7, top], {"xlo": xo}),
        (W.at[6, low], W.at[7, low], {"xlo": xo}),
    )

    def w_send(n):
        src, dst, dev = wspec[n]
        return rcopy(src, dst, ws.at[n], wr.at[n], dev)

    up, dn = pl.ds(0, 256), pl.ds(256, 256)
    rspec = (
        (S.at[0], RX.at[0], {"xlo": xo}),
        (S.at[1, up], RH.at[0], {"y": yp}),
        (S.at[1, dn], RH.at[1], {"y": ym}),
        (S.at[2], RP.at[0], {"y": yp}),
        (S.at[3], RP.at[1], {"y": ym}),
        (S.at[4, dn], RY.at[0, dn], {"y": yp}),
        (S.at[5, up], RY.at[1, up], {"y": ym}),
        (S.at[4, up], RY.at[0, up], {"y": yp}),
        (S.at[5, dn], RY.at[1, dn], {"y": ym}),
        (S.at[6], RX.at[1], {"xlo": xo}),
    )

    def r_send(n):
        src, dst, dev = rspec[n]
        return rcopy(src, dst, rs.at[n], rr.at[n], dev)

    def add_into(dst, rows, srcs):
        @pl.loop(0, rows // 64)
        def _(n):
            at = pl.ds(pl.multiple_of(n * 64, 64), 64)
            total = dst[at].astype(F32)
            for src in srcs:
                total = total + src[at].astype(F32)
            dst[at] = total.astype(BF)

    def weight_part(j):
        @pl.loop(0, 4)
        def _(n):
            at = pl.ds(pl.multiple_of(n * 256, 256), 256)
            rows = G[j, :, :, :, :, at].reshape(1024, 256)
            S[j, :, at] = dot(AT[...], rows).astype(BF)

    def att_part(j):
        @pl.loop(0, 2)
        def _(a):
            @pl.loop(0, 2)
            def _(b):
                at = pl.ds(pl.multiple_of((a * 2 + b) * 256, 256), 256)
                rows = G[j, a, pl.ds(b * 2, 2)].reshape(256, 1024)
                ACC[at] += dot(rows, W[7 - j])

    def w_start(*which):
        for n in which:
            w_send(n).start()

    def w_wait(*which):
        for n in which:
            w_send(n).wait_recv()

    for cp in own:
        cp.wait()
    wcp.wait()
    for j in range(2):
        for d in range(2):
            u_send(j, d, 0).start()
    w_start(0, 1, 2, 3)
    for j in range(4):
        x_send(j).start()
    w_start(4)
    for j in range(4, 6):
        x_send(j).start()
    w_start(5)
    for j in range(6, 8):
        x_send(j).start()
    acp.wait()
    for h in range(4):
        AT[h * HD : (h + 1) * HD] = A[:, h * HD : (h + 1) * HD].T
    for cp in others:
        cp.wait()
    KT[...] = K[...].T
    ACC[...] = jnp.zeros_like(ACC)
    DK[...] = jnp.zeros_like(DK)
    DV[...] = jnp.zeros_like(DV)

    def spans(b):
        n, lo = (b + 1) * 256, b * 256
        return n, lo

    def prob_part(h):
        for b in range(4):
            n, lo = spans(b)
            scores = dot(K[:n], Q[h, lo:n], NT) * scale
            keys_at = lax.broadcasted_iota(jnp.int32, (n, 256), 0)
            query_at = lax.broadcasted_iota(jnp.int32, (n, 256), 1) + lo
            stat = ST[pl.ds(h, 1), lo:n]
            PT[b][h] = jnp.where(keys_at <= query_at, jnp.exp(scores - stat), 0.0).astype(BF)

    @pl.loop(0, 11)
    def _(i):
        @pl.when(i < 8)
        def _():
            x_recv(i).wait_recv()
            u_send(i, 0, 1).start()
            u_send(i, 1, 1).start()
            c_send(i, 0).start()

        @pl.when(i >= 3)
        def _():
            j = i - 3
            for s in range(4):
                c_recv(j, s).wait_recv()
            weight_part(j)

        @pl.when(i == 3)
        def _():
            r_send(0).start()

        @pl.when(i == 5)
        def _():
            r_send(3).start()

        @pl.when(i == 6)
        def _():
            r_send(4).start()

        @pl.when((i >= 1) & (i < 5))
        def _():
            prob_part(i - 1)

        @pl.when((i >= 1) & (i < 9))
        def _():
            j = i - 1
            for d in range(2):
                u_recv(j, d, 0).wait_recv()
                u_recv(j, d, 1).wait_recv()
                z_send(j, d).start()
            c_send(j, 1).start()
            c_send(j, 2).start()

        @pl.when(i < 6)
        def _():
            for d in range(2):
                u_send(i + 2, d, 0).start()

        @pl.when(i == 2)
        def _():
            w_wait(0, 1)
            w_start(6, 7)

        @pl.when((i >= 2) & (i < 10))
        def _():
            j = i - 2
            for d in range(2):
                z_recv(j, d).wait_recv()
            c_send(j, 3).start()

        @pl.when(i == 3)
        def _():
            w_wait(4)
            w_start(8, 9)

        @pl.when(i == 4)
        def _():
            w_wait(2, 3, 6, 7)
            w_start(12, 13)
            w_wait(5)
            w_start(10, 11)

        @pl.when(i == 8)
        def _():
            w_wait(8, 9, 10, 11)

        @pl.when(i >= 7)
        def _():
            att_part(i - 3)

        @pl.when((i >= 7) & (i < 10))
        def _():
            att_part(i - 6)

        @pl.when(i == 9)
        def _():
            r_send(0).wait_recv()
            add_into(S.at[1], 512, [RX.at[0]])
            for n in (1, 2, 5, 6):
                r_send(n).start()

    r_send(3).wait_recv()
    r_send(4).wait_recv()
    add_into(S.at[6], 512, [RP.at[0], RP.at[1]])
    r_send(9).start()

    w_wait(12, 13)
    att_part(0)

    for h in range(4):
        part = ACC[:, h * HD : (h + 1) * HD].astype(BF)
        GA[h] = part
        GAT[h] = part.T

    def r_mid():
        r_send(1).wait_recv()
        add_into(S.at[4, up], 256, [RH.at[0]])
        r_send(7).start()
        r_send(2).wait_recv()
        add_into(S.at[5, dn], 256, [RH.at[1]])
        r_send(8).start()

    @pl.loop(0, 4)
    def _(h):
        @pl.when(h == 1)
        def _():
            r_mid()

        for b in range(4):
            n, lo = spans(b)
            qb = Q[h, lo:n]
            gb = GA[h, lo:n]
            gt = GAT[h, :, lo:n]
            at_rows = AT[pl.ds(pl.multiple_of(h * HD, HD), HD), lo:n]
            offset = jnp.sum(gt.astype(F32) * at_rows.astype(F32), axis=0, keepdims=True)
            attention = PT[b][h]
            DV[:n] += dot(attention, gb)
            grad_att = dot(V[:n], gb, NT)
            grad_scores = (attention.astype(F32) * (grad_att - offset)).astype(BF)
            DK[:n] += dot(grad_scores, qb)
            dq = dot(KT[:, :n], grad_scores) * scale
            dq_out[lo:n, pl.ds(pl.multiple_of(h * HD, HD), HD)] = dq.T.astype(BF)

    zh = lax.rem(z, 2)
    dkt = (DK[...] * scale).T
    dvt = DV[...].T
    for n, full in enumerate((dkt, dvt)):
        for half in range(2):
            piece = full[half * 64 : half * 64 + 64]
            KF[n, half] = piece
            KB[half, n] = piece.astype(BF)
    k_send1 = rcopy(KB.at[1 - zh], KR1, ks.at[0], kr.at[0], {"z": zpair})
    k_send1.start()
    k_send1.wait_recv()
    for n in range(2):
        kept = KF[n, zh] + KR1[n].astype(F32)
        KF[n, 0] = kept
        KB2[0, n] = kept[:32].astype(BF)
        KB2[1, n] = kept[32:].astype(BF)
    k_send2 = rcopy(KB2.at[1 - c], KR2, ks.at[1], kr.at[1], {"core": co})
    k_send2.start()
    k_send2.wait_recv()
    for n in range(2):
        kv_out[n] = (KF[n, 0, pl.ds(pl.multiple_of(c * 32, 32), 32)] + KR2[n].astype(F32)).astype(BF)

    for n in (5, 6, 7, 8, 9):
        r_send(n).wait_recv()

    @pl.loop(0, 8)
    def _(n):
        at = pl.ds(pl.multiple_of(n * 64, 64), 64)
        total = S[7, at].astype(F32)
        for src in (RY.at[0], RY.at[1], RX.at[1]):
            total = total + src[at].astype(F32)
        wg_out[at] = total.astype(BF)

    @pl.loop(0, 8)
    def _(j):
        x_send(j).wait_send()
        for d in range(2):
            u_send(j, d, 0).wait_send()
            u_send(j, d, 1).wait_send()
            z_send(j, d).wait_send()
        for s in range(4):
            c_send(j, s).wait_send()

    for n in range(14):
        w_send(n).wait_send()
    for n in range(10):
        r_send(n).wait_send()
    k_send1.wait_send()
    k_send2.wait_send()


def finish(dq_in, kv_in, wg_in, dq_out, dk_out, dv_out, wg_out):
    for n in range(4):
        wg_out[:, n * HD : (n + 1) * HD] = wg_in[n * HD : (n + 1) * HD].T
    dq_out[...] = dq_in[...]
    dk_out[...] = kv_in[0]
    dv_out[...] = kv_in[1]


def per_device(grad_out, out_weight, query, keys, values, attended, stats):
    any_spec = pl.BlockSpec(memory_space=pl.ANY)
    vmem = pl.BlockSpec(memory_space=pltpu.VMEM)
    V_ = pltpu.VMEM
    dma = pltpu.SemaphoreType.DMA
    scratch = [
        V_((8, 2, 4, 2, 64, 1024), BF),
        V_((8, 1024, 512), BF),
        V_((8, 512, 1024), BF),
        V_((2, 512, 1024), BF),
        V_((2, 256, 1024), BF),
        V_((2, 512, 1024), BF),
        V_((2, 512, 1024), BF),
        V_((512, 1024), BF),
        V_((1024, 512), F32),
        V_((4, 1024, HD), BF),
        V_((4, 1024, HD), BF),
        V_((4, HD, 1024), BF),
        V_((1024, HD), BF),
        V_((1024, HD), BF),
        V_((HD, 1024), BF),
        V_((1024, 512), BF),
        V_((4, 1024), F32),
        V_((4, 256, 256), BF),
        V_((4, 512, 256), BF),
        V_((4, 768, 256), BF),
        V_((4, 1024, 256), BF),
        V_((1024, HD), F32),
        V_((1024, HD), F32),
        V_((2, 2, 64, 1024), F32),
        V_((2, 2, 64, 1024), BF),
        V_((2, 64, 1024), BF),
        V_((2, 2, 32, 1024), BF),
        V_((2, 32, 1024), BF),
        dma((8,)), dma((8,)),
        dma((8, 2, 2)), dma((8, 2, 2)),
        dma((8, 2)), dma((8, 2)),
        dma((8, 4)), dma((8, 4)),
        dma((14,)), dma((14,)),
        dma((10,)), dma((10,)),
        dma((2,)), dma((2,)),
        dma((8,)), dma((9,)),
    ]
    dq, kv, wg = pl.pallas_call(
        kernel,
        out_shape=(
            jax.ShapeDtypeStruct((1024, 512), BF),
            jax.ShapeDtypeStruct((2, 32, 1024), BF),
            jax.ShapeDtypeStruct((512, 1024), BF),
        ),
        in_specs=[any_spec] * 7,
        out_specs=(vmem, vmem, vmem),
        scratch_shapes=scratch,
        compiler_params=pltpu.CompilerParams(
            collective_id=0, has_side_effects=True, vmem_limit_bytes=67_000_000
        ),
    )(grad_out, out_weight, query, keys, values, attended, stats)
    dq, dk, dv, wg = pl.pallas_call(
        finish,
        out_shape=(
            jax.ShapeDtypeStruct((1024, 512), BF),
            jax.ShapeDtypeStruct((32, 1024), BF),
            jax.ShapeDtypeStruct((32, 1024), BF),
            jax.ShapeDtypeStruct((1024, 512), BF),
        ),
        in_specs=[vmem] * 3,
        out_specs=(vmem,) * 4,
    )(dq, kv, wg)
    return (dq, dk.T, dv.T, wg)


def solution(mesh):
    torus = Mesh(mesh.devices.reshape(4, 2, 2, 4, 2), AXES)
    dp, tp = ("y", "xlo"), ("xhi", "z", "core")
    in_specs = (
        P(dp + tp, None),
        P(dp, tp),
        P(dp, tp),
        P(dp, None),
        P(dp, None),
        P(dp, tp),
        P(tp, dp),
    )
    out_specs = (P(dp, tp), P(dp, tp), P(dp, tp), P(dp, tp))
    return jax.shard_map(
        per_device, mesh=torus, in_specs=in_specs, out_specs=out_specs, check_vma=False
    )
```

```python
import jax
import jax.numpy as jnp
from jax import lax
from jax.experimental import pallas as pl
from jax.experimental.pallas import tpu as pltpu
from jax.sharding import Mesh
from jax.sharding import PartitionSpec as P

HD = 128
GROUP = 16
BF = jnp.bfloat16
F32 = jnp.float32
AXES = ("y", "xlo", "xhi", "z", "core")
NN = (((1,), (0,)), ((), ()))
NT = (((1,), (1,)), ((), ()))


def dot(a, b, dims=NN):
    return lax.dot_general(a, b, dims, preferred_element_type=F32)


def rcopy(src, dst, send, recv, dev):
    return pltpu.make_async_remote_copy(
        src_ref=src,
        dst_ref=dst,
        send_sem=send,
        recv_sem=recv,
        device_id=dev,
        device_id_type=pl.DeviceIdType.MESH,
    )


def kernel(
    g_in, w_in, q_in, k_in, v_in, a_in, st_in,
    dq_out, dk_out, dv_out, wg_out,
    G, W, S, RH, RY, AT, AT2, ACC, PG, PS, PR, Q, GA, OFF, K, V, KT, ST,
    P0, P1, P2, P3, DQ, KF, KB, KS, KR1, KB2, KR2,
    xs, xr, es, er, us, ur, zs, zr, cs, cr, ws, wr, rs, rr, ats, atr, ps, pr, ks, kr, ls,
):
    y, xlo, xhi = lax.axis_index("y"), lax.axis_index("xlo"), lax.axis_index("xhi")
    z, c = lax.axis_index("z"), lax.axis_index("core")
    scale = HD ** (-0.5)
    PT = (P0, P1, P2, P3)
    yp, ym, y2 = lax.rem(y + 1, 4), lax.rem(y + 3, 4), lax.rem(y + 2, 4)
    zp, zm, z2 = lax.rem(z + 1, 4), lax.rem(z + 3, 4), lax.rem(z + 2, 4)
    xo, xh, co = 1 - xlo, 1 - xhi, 1 - c
    zpair = z + 1 - 2 * lax.rem(z, 2)

    head = xhi * 2 + z // 2
    hcol = pl.ds(pl.multiple_of(head * HD, HD), HD)
    blocks = (y2, yp, ym, y)
    own_chunk = (0, 5, 6, 7)
    pair_chunk = (1, 2, 3, 4)

    def columns(q, x):
        return pl.ds(pl.multiple_of((blocks[q] * 2 + x) * 1024, 1024), 1024)

    for q in range(4):
        pltpu.make_async_copy(
            g_in.at[:, columns(q, xlo)], G.at[own_chunk[q], xhi, z, c], ls.at[0]
        ).start()
    wcp = pltpu.make_async_copy(w_in, W.at[0], ls.at[1])
    wcp.start()
    for h in range(4):
        pltpu.make_async_copy(a_in.at[:, h * HD : (h + 1) * HD], GA.at[h], ls.at[2]).start()
        pltpu.make_async_copy(q_in.at[:, h * HD : (h + 1) * HD], Q.at[h], ls.at[3]).start()
    others = [
        pltpu.make_async_copy(k_in.at[:, hcol], K, ls.at[4]),
        pltpu.make_async_copy(v_in.at[:, hcol], V, ls.at[5]),
        pltpu.make_async_copy(st_in, ST, ls.at[6]),
    ]
    for cp in others:
        cp.start()

    barrier = pltpu.get_barrier_semaphore()
    for dev in ({"y": yp}, {"y": ym}, {"xlo": xo}, {"xhi": xh}, {"z": zp}, {"z": zm}, {"core": co}):
        pl.semaphore_signal(barrier, inc=1, device_id=dev, device_id_type=pl.DeviceIdType.MESH)
    pl.semaphore_wait(barrier, 7)

    def e_send(q):
        dst = G.at[pair_chunk[q], xhi, z, c]
        return rcopy(g_in.at[:, columns(q, xo)], dst, es, er.at[q], {"xlo": xo})

    def e_recv(q):
        dst = G.at[pair_chunk[q], xhi, z, c]
        return rcopy(dst, dst, es, er.at[q], {"xlo": xo})

    def x_send(j):
        return rcopy(G.at[j, xhi, z, c], G.at[j, xhi, z, c], xs, xr.at[j], {"xhi": xh})

    def x_recv(j):
        return rcopy(G.at[j, xh, z, c], G.at[j, xh, z, c], xs, xr.at[j], {"xhi": xh})

    def unit(j, zz, cc):
        return G.at[j, :, zz, cc]

    def u_send(j, d, p):
        at = G.at[j, (xhi, xh)[p], z, c]
        return rcopy(at, at, us, ur.at[j, d], {"z": (zp, zm)[d]})

    def u_recv(j, d):
        at = unit(j, (zm, zp)[d], c)
        return rcopy(at, at, us, ur.at[j, d], {"z": (zp, zm)[d]})

    def z_send(j, d):
        at = G.at[j, d, (zm, zp)[d], c]
        return rcopy(at, at, zs, zr.at[j], {"z": (zp, zm)[d]})

    def z_recv(j):
        at = unit(j, z2, c)
        return rcopy(at, at, zs, zr.at[j], {"z": zp})

    slots = (z, zm, zp, z2)

    def c_send(j, s):
        at = unit(j, slots[s], c)
        return rcopy(at, at, cs, cr.at[j], {"core": co})

    def c_recv(j):
        at = G.at[j, :, :, co]
        return rcopy(at, at, cs, cr.at[j], {"core": co})

    top, low = pl.ds(0, 512), pl.ds(512, 512)
    wspec = (
        (W.at[0, top], W.at[1, top], {"y": yp}),
        (W.at[0, low], W.at[2, low], {"y": ym}),
        (W.at[0, low], W.at[1, low], {"y": yp}),
        (W.at[0, top], W.at[2, top], {"y": ym}),
        (W.at[1, top], W.at[3, top], {"y": yp}),
        (W.at[2, low], W.at[3, low], {"y": ym}),
    )

    def w_send(n):
        src, dst, dev = wspec[n]
        return rcopy(src, dst, ws, wr.at[n], dev)

    up, dn = pl.ds(0, 256), pl.ds(256, 256)
    rspec = (
        (S.at[0, up], RH.at[0], {"y": yp}),
        (S.at[0, dn], RH.at[1], {"y": ym}),
        (S.at[1, dn], RY.at[0, dn], {"y": yp}),
        (S.at[1, up], RY.at[0, up], {"y": yp}),
        (S.at[2, up], RY.at[1, up], {"y": ym}),
        (S.at[2, dn], RY.at[1, dn], {"y": ym}),
    )

    def r_send(n):
        src, dst, dev = rspec[n]
        return rcopy(src, dst, rs, rr.at[n], dev)

    def a_send(h):
        at = pl.ds(h * HD, HD)
        return rcopy(AT.at[at], AT2.at[at], ats, atr.at[h], {"xlo": xo})

    def p_send():
        return rcopy(PS, PR, ps, pr, {"xlo": xo})

    def add_into(dst, rows, srcs):
        @pl.loop(0, rows // 64)
        def _(n):
            at = pl.ds(pl.multiple_of(n * 64, 64), 64)
            total = dst[at].astype(F32)
            for src in srcs:
                total = total + src[at].astype(F32)
            dst[at] = total.astype(BF)

    def weight_part(q, rows):
        @pl.loop(0, 4)
        def _(n):
            at = pl.ds(pl.multiple_of(n * 256, 256), 256)
            mine = G[own_chunk[q], :, :, :, :, at].reshape(1024, 256)
            pair = G[pair_chunk[q], :, :, :, :, at].reshape(1024, 256)
            S[q, rows, at] = (dot(AT[rows], mine) + dot(AT2[rows], pair)).astype(BF)

    def att_part(acc, j, slot):
        @pl.loop(0, 2)
        def _(a):
            @pl.loop(0, 2)
            def _(b):
                at = pl.ds(pl.multiple_of((a * 2 + b) * 256, 256), 256)
                rows = G[j, a, pl.ds(b * 2, 2)].reshape(256, 1024)
                acc[at] += dot(rows, W[slot])

    def w_start(*which):
        for n in which:
            w_send(n).start()

    def w_wait(*which):
        for n in which:
            w_send(n).wait_recv()

    first = G.at[pl.ds(0, 4), 0, 0, 0]
    pltpu.make_async_copy(first, first, ls.at[0]).wait()
    wcp.wait()
    for d in range(2):
        u_send(0, d, 0).start()
    w_start(0, 1, 2, 3)
    x_send(0).start()
    e_send(0).start()
    e_send(1).start()
    pltpu.make_async_copy(GA, GA, ls.at[2]).wait()
    for h in range(4):
        AT[h * HD : (h + 1) * HD] = GA[h].T
    pltpu.make_async_copy(Q, Q, ls.at[3]).wait()
    for cp in others:
        cp.wait()
    KT[...] = K[...].T
    ACC[...] = jnp.zeros_like(ACC)
    PG[...] = jnp.zeros_like(PG)

    def prob_part(h):
        stat = ST[pl.ds(h, 1)]
        for r in range(4):
            lo = r * 256
            n = 1024 - lo
            scores = dot(K[lo : lo + 256], Q[h, lo:], NT) * scale
            keys_at = lax.broadcasted_iota(jnp.int32, (256, n), 0)
            query_at = lax.broadcasted_iota(jnp.int32, (256, n), 1)
            value = jnp.exp(scores - stat[:, lo:])
            PT[r][h] = jnp.where(keys_at <= query_at, value, 0.0).astype(BF)

    def at_step(i, n, run):
        @pl.when(i == n)
        def _():
            run()

    @pl.loop(0, 11)
    def _(i):
        @pl.when(i < 8)
        def _():
            x_recv(i).wait_recv()
            u_send(i, 0, 1).start()
            u_send(i, 1, 1).start()
            c_send(i, 0).start()

        def feed(q):
            e_recv(q).wait_recv()
            x_send(q + 1).start()
            for d in range(2):
                u_send(q + 1, d, 0).start()

        def feed_0():
            feed(0)
            e_send(2).start()

        def feed_1():
            feed(1)
            e_send(3).start()
            a_send(0).start()

        def feed_2():
            feed(2)
            a_send(1).start()

        def feed_3():
            feed(3)
            a_send(2).start()
            x_send(5).start()

        def feed_4():
            a_send(3).start()
            x_send(6).start()

        def feed_5():
            x_send(7).start()

        for n, run in enumerate((feed_0, feed_1, feed_2, feed_3, feed_4, feed_5)):
            at_step(i, n, run)

        @pl.when(i >= 3)
        def _():
            c_recv(i - 3).wait_recv()

        def pair_done():
            att_part(PG, 4, 0)
            PS[...] = PG[...].astype(BF)
            p_send().start()

        at_step(i, 7, pair_done)

        @pl.when((i >= 1) & (i < 5))
        def _():
            prob_part(i - 1)

        @pl.when((i >= 1) & (i < 9))
        def _():
            j = i - 1
            for d in range(2):
                u_recv(j, d).wait_recv()
                z_send(j, d).start()
            c_send(j, 1).start()
            c_send(j, 2).start()

        @pl.when((i >= 4) & (i < 7))
        def _():
            for d in range(2):
                u_send(i + 1, d, 0).start()

        def relay_w():
            w_wait(0, 1)
            w_start(4, 5)

        at_step(i, 2, relay_w)

        @pl.when((i >= 2) & (i < 10))
        def _():
            j = i - 2
            z_recv(j).wait_recv()
            c_send(j, 3).start()

        def step_4():
            w_wait(2, 3, 4, 5)
            att_part(ACC, 0, 3)

        def step_5():
            a_send(0).wait_recv()
            a_send(1).wait_recv()
            weight_part(0, up)
            r_send(0).start()
            att_part(PG, 1, 3)
            att_part(PG, 2, 2)

        def step_6():
            att_part(PG, 3, 1)
            a_send(2).wait_recv()
            a_send(3).wait_recv()
            weight_part(0, dn)
            r_send(1).start()

        def step_8():
            weight_part(1, pl.ds(0, 512))
            r_send(2).start()
            r_send(0).wait_recv()
            add_into(S.at[1, up], 256, [RH.at[0]])
            r_send(3).start()
            att_part(ACC, 5, 2)

        def step_9():
            weight_part(2, pl.ds(0, 512))
            r_send(4).start()
            r_send(1).wait_recv()
            add_into(S.at[2, dn], 256, [RH.at[1]])
            r_send(5).start()
            att_part(ACC, 6, 1)

        def step_10():
            att_part(ACC, 7, 0)
            weight_part(3, pl.ds(0, 512))

        for n, run in ((4, step_4), (5, step_5), (6, step_6), (8, step_8), (9, step_9), (10, step_10)):
            at_step(i, n, run)

    p_send().wait_recv()
    for h in range(4):
        cols = slice(h * HD, (h + 1) * HD)
        part = (ACC[:, cols] + PR[:, cols].astype(F32)).astype(BF)
        GA[h] = part
        both = part.T.astype(F32) * AT[h * HD : (h + 1) * HD].astype(F32)
        OFF[h : h + 1] = jnp.sum(both, axis=0, keepdims=True)

    zh = lax.rem(z, 2)

    def kv_first(r):
        return rcopy(KB.at[r, :, :, 1 - c], KR1.at[r], ks.at[0], kr.at[0, r], {"core": co})

    def kv_second(r):
        return rcopy(KB2.at[r, 1 - zh], KR2.at[r], ks.at[1], kr.at[1, r], {"z": zpair})

    def kv_middle(r):
        kv_first(r).wait_recv()
        for n in range(2):
            for half in range(2):
                total = KF[r, n, half, c] + KR1[r, n, half].astype(F32)
                KS[r, n, half] = total
                KB2[r, half, n] = total.astype(BF)
        kv_second(r).start()

    for r in range(4):
        lo = r * 256
        mine = slice(lo, lo + 256)
        dv = jnp.zeros((256, HD), F32)
        dk = jnp.zeros((256, HD), F32)
        for h in range(4):
            attention = PT[r][h]
            gb = GA[h, lo:]
            dv = dv + dot(attention, gb)
            grad_att = dot(V[mine], gb, NT)
            grad_scores = (attention.astype(F32) * (grad_att - OFF[h : h + 1, lo:])).astype(BF)
            dk = dk + dot(grad_scores, Q[h, lo:])
            dq = dot(KT[:, mine], grad_scores)
            if r > 0:
                dq = dq + DQ[h, :, lo:]
            DQ[h, :, lo:] = dq
            dq_out[mine, h * HD : (h + 1) * HD] = (dq[:, :256] * scale).T.astype(BF)
        for n, full in enumerate(((dk * scale).T, dv.T)):
            for half in range(2):
                for core in range(2):
                    at = half * 64 + core * 32
                    KF[r, n, half, core] = full[at : at + 32]
                    KB[r, n, half, core] = full[at : at + 32].astype(BF)
        kv_first(r).start()
        if r > 0:
            kv_middle(r - 1)
    kv_middle(3)
    for r in range(4):
        kv_second(r).wait_recv()
        for n in range(2):
            total = KS[r, n, zh] + KR2[r, n].astype(F32)
            (dk_out, dv_out)[n][:, r * 256 : r * 256 + 256] = total.astype(BF)

    r_send(2).wait_recv()
    r_send(3).wait_recv()
    for n in range(4):
        at = slice(n * HD, (n + 1) * HD)
        ACC[:, at] = (S[3, at].astype(F32) + RY[0, at].astype(F32)).T
    for n in range(4):
        at = slice(n * HD, (n + 1) * HD)
        if n % 2 == 0:
            r_send(4 + n // 2).wait_recv()
        wg_out[:, at] = (ACC[:, at] + RY[1, at].T.astype(F32)).astype(BF)

    for ref, sem in (
        (first, es),
        (G.at[:, 0, 0, 0], xs),
        (G.at[pl.ds(0, 2)], us),
        (G.at[0], zs),
        (G.at[pl.ds(0, 4)], cs),
        (W.at[pl.ds(0, 3)], ws),
        (S.at[pl.ds(0, 3)], rs),
        (AT, ats),
        (PS, ps),
        (KR1, ks.at[0]),
        (KR2, ks.at[1]),
    ):
        rcopy(ref, ref, sem, sem, {"core": co}).wait_send()


def finish(*refs):
    sems = refs[8]
    copies = [pltpu.make_async_copy(refs[n], refs[4 + n], sems.at[n]) for n in range(4)]
    for cp in copies:
        cp.start()
    for cp in copies:
        cp.wait()


def per_device(grad_out, out_weight, query, keys, values, attended, stats):
    any_spec = pl.BlockSpec(memory_space=pl.ANY)
    vmem = pl.BlockSpec(memory_space=pltpu.VMEM)
    V_ = pltpu.VMEM
    dma = pltpu.SemaphoreType.DMA
    scratch = [
        V_((8, 2, 4, 2, 64, 1024), BF),
        V_((4, 1024, 512), BF),
        V_((4, 512, 1024), BF),
        V_((2, 256, 1024), BF),
        V_((2, 512, 1024), BF),
        V_((512, 1024), BF),
        V_((512, 1024), BF),
        V_((1024, 512), F32),
        V_((1024, 512), F32),
        V_((1024, 512), BF),
        V_((1024, 512), BF),
        V_((4, 1024, HD), BF),
        V_((4, 1024, HD), BF),
        V_((4, 1024), F32),
        V_((1024, HD), BF),
        V_((1024, HD), BF),
        V_((HD, 1024), BF),
        V_((4, 1024), F32),
        V_((4, 256, 1024), BF),
        V_((4, 256, 768), BF),
        V_((4, 256, 512), BF),
        V_((4, 256, 256), BF),
        V_((4, HD, 1024), F32),
        V_((4, 2, 2, 2, 32, 256), F32),
        V_((4, 2, 2, 2, 32, 256), BF),
        V_((4, 2, 2, 32, 256), F32),
        V_((4, 2, 2, 32, 256), BF),
        V_((4, 2, 2, 32, 256), BF),
        V_((4, 2, 32, 256), BF),
        dma, dma((8,)),
        dma, dma((4,)),
        dma, dma((8, 2)),
        dma, dma((8,)),
        dma, dma((8,)),
        dma, dma((6,)),
        dma, dma((6,)),
        dma, dma((4,)),
        dma, dma,
        dma((2,)), dma((2, 4)),
        dma((7,)),
    ]
    dq, dk, dv, wg = pl.pallas_call(
        kernel,
        out_shape=(
            V_((1024, 512), BF),
            V_((32, 1024), BF),
            V_((32, 1024), BF),
            V_((1024, 512), BF),
        ),
        in_specs=[any_spec] * 7,
        out_specs=(vmem,) * 4,
        scratch_shapes=scratch,
        compiler_params=pltpu.CompilerParams(
            collective_id=0, has_side_effects=True, vmem_limit_bytes=58_700_000
        ),
    )(grad_out, out_weight, query, keys, values, attended, stats)
    results = (dq, dk, dv, wg)
    dq, dk, dv, wg = pl.pallas_call(
        finish,
        out_shape=tuple(jax.ShapeDtypeStruct(r.shape, r.dtype) for r in results),
        in_specs=[any_spec] * 4,
        out_specs=(any_spec,) * 4,
        scratch_shapes=[dma((4,))],
        compiler_params=pltpu.CompilerParams(vmem_limit_bytes=1 << 20),
    )(*results)
    return (dq, dk.T, dv.T, wg)


def solution(mesh):
    torus = Mesh(mesh.devices.reshape(4, 2, 2, 4, 2), AXES)
    dp, tp = ("y", "xlo"), ("xhi", "z", "core")
    in_specs = (
        P(dp + tp, None),
        P(dp, tp),
        P(dp, tp),
        P(dp, None),
        P(dp, None),
        P(dp, tp),
        P(tp, dp),
    )
    out_specs = (P(dp, tp), P(dp, tp), P(dp, tp), P(dp, tp))
    return jax.shard_map(
        per_device, mesh=torus, in_specs=in_specs, out_specs=out_specs, check_vma=False
    )
```

```python
import jax
import jax.numpy as jnp
from jax import lax
from jax.experimental import pallas as pl
from jax.experimental.pallas import tpu as pltpu
from jax.sharding import Mesh
from jax.sharding import PartitionSpec as P

HD = 128
GROUP = 16
BF = jnp.bfloat16
F32 = jnp.float32
AXES = ("y", "xlo", "xhi", "z", "core")
NN = (((1,), (0,)), ((), ()))
NT = (((1,), (1,)), ((), ()))


def dot(a, b, dims=NN):
    return lax.dot_general(a, b, dims, preferred_element_type=F32)


def rcopy(src, dst, send, recv, dev):
    return pltpu.make_async_remote_copy(
        src_ref=src,
        dst_ref=dst,
        send_sem=send,
        recv_sem=recv,
        device_id=dev,
        device_id_type=pl.DeviceIdType.MESH,
    )


def kernel(
    g_in, w_in, q_in, k_in, v_in, a_in, st_in,
    dq_out, dk_out, dv_out, wg_out,
    G, W, S, RH, RY, AT, AT2, ACC, PG, PS, PR, Q, GA, OFF, K, V, KT, ST,
    P0, P1, P2, P3, DQ, KF, KB, KS, KR1, KB2, KR2,
    xs, xr, es, er, us, ur, zs, zr, cs, cr, ws, wr, rs, rr, ats, atr, ps, pr, ks, kr, ls,
):
    y, xlo, xhi = lax.axis_index("y"), lax.axis_index("xlo"), lax.axis_index("xhi")
    z, c = lax.axis_index("z"), lax.axis_index("core")
    scale = HD ** (-0.5)
    PT = (P0, P1, P2, P3)
    yp, ym, y2 = lax.rem(y + 1, 4), lax.rem(y + 3, 4), lax.rem(y + 2, 4)
    zp, zm, z2 = lax.rem(z + 1, 4), lax.rem(z + 3, 4), lax.rem(z + 2, 4)
    xo, xh, co = 1 - xlo, 1 - xhi, 1 - c
    zpair = z + 1 - 2 * lax.rem(z, 2)

    head = xhi * 2 + z // 2
    hcol = pl.ds(pl.multiple_of(head * HD, HD), HD)
    blocks = (y2, yp, ym, y)
    pair_chunk = (1, 2, 3, 4)

    def columns(q, x, first=0, count=1024):
        return pl.ds(pl.multiple_of((blocks[q] * 2 + x) * 1024 + first, 512), count)

    for q, j in ((0, 0), (3, 7)):
        pltpu.make_async_copy(
            g_in.at[:, columns(q, xlo)], G.at[j, xhi, z, c], ls.at[0]
        ).start()
    for q in (1, 2):
        for half in range(2):
            at = pl.ds((q - 1) * 512, 512)
            pltpu.make_async_copy(
                g_in.at[:, columns(q, xlo, half * 512, 512)],
                G.at[5 + half, xhi, z, c, :, at],
                ls.at[0],
            ).start()
    wcp = pltpu.make_async_copy(w_in, W.at[0], ls.at[1])
    wcp.start()
    for h in range(4):
        pltpu.make_async_copy(a_in.at[:, h * HD : (h + 1) * HD], GA.at[h], ls.at[2]).start()
        pltpu.make_async_copy(q_in.at[:, h * HD : (h + 1) * HD], Q.at[h], ls.at[3]).start()
    others = [
        pltpu.make_async_copy(k_in.at[:, hcol], K, ls.at[4]),
        pltpu.make_async_copy(v_in.at[:, hcol], V, ls.at[5]),
        pltpu.make_async_copy(st_in, ST, ls.at[6]),
    ]
    for cp in others:
        cp.start()

    barrier = pltpu.get_barrier_semaphore()
    for dev in ({"y": yp}, {"y": ym}, {"xlo": xo}, {"xhi": xh}, {"z": zp}, {"z": zm}, {"core": co}):
        pl.semaphore_signal(barrier, inc=1, device_id=dev, device_id_type=pl.DeviceIdType.MESH)
    pl.semaphore_wait(barrier, 7)

    def e_send(q):
        dst = G.at[pair_chunk[q], xhi, z, c]
        return rcopy(g_in.at[:, columns(q, xo)], dst, es, er.at[q], {"xlo": xo})

    def e_recv(q):
        dst = G.at[pair_chunk[q], xhi, z, c]
        return rcopy(dst, dst, es, er.at[q], {"xlo": xo})

    def x_send(j):
        return rcopy(G.at[j, xhi, z, c], G.at[j, xhi, z, c], xs, xr.at[j], {"xhi": xh})

    def x_recv(j):
        return rcopy(G.at[j, xh, z, c], G.at[j, xh, z, c], xs, xr.at[j], {"xhi": xh})

    def unit(j, zz, cc):
        return G.at[j, :, zz, cc]

    def u_send(j, d, p):
        at = G.at[j, (xhi, xh)[p], z, c]
        return rcopy(at, at, us, ur.at[j, d], {"z": (zp, zm)[d]})

    def u_recv(j, d):
        at = unit(j, (zm, zp)[d], c)
        return rcopy(at, at, us, ur.at[j, d], {"z": (zp, zm)[d]})

    def z_send(j, d):
        at = G.at[j, d, (zm, zp)[d], c]
        return rcopy(at, at, zs, zr.at[j], {"z": (zp, zm)[d]})

    def z_recv(j):
        at = unit(j, z2, c)
        return rcopy(at, at, zs, zr.at[j], {"z": zp})

    slots = (z, zm, zp, z2)

    def c_send(j, s):
        at = unit(j, slots[s], c)
        return rcopy(at, at, cs, cr.at[j], {"core": co})

    def c_recv(j):
        at = G.at[j, :, :, co]
        return rcopy(at, at, cs, cr.at[j], {"core": co})

    top, low = pl.ds(0, 512), pl.ds(512, 512)
    wspec = (
        (W.at[0, top], W.at[1, top], {"y": yp}),
        (W.at[0, low], W.at[2, low], {"y": ym}),
        (W.at[0, low], W.at[1, low], {"y": yp}),
        (W.at[0, top], W.at[2, top], {"y": ym}),
        (W.at[1, top], W.at[3, top], {"y": yp}),
        (W.at[2, low], W.at[3, low], {"y": ym}),
    )

    def w_send(n):
        src, dst, dev = wspec[n]
        return rcopy(src, dst, ws, wr.at[n], dev)

    up, dn = pl.ds(0, 256), pl.ds(256, 256)
    rspec = (
        (S.at[0, up], RH.at[0], {"y": yp}),
        (S.at[0, dn], RH.at[1], {"y": ym}),
        (S.at[1, :, top], RY.at[0, :, top], {"y": yp}),
        (S.at[1, :, low], RY.at[0, :, low], {"y": yp}),
        (S.at[2, up, top], RY.at[1, up, top], {"y": ym}),
        (S.at[2, up, low], RY.at[1, up, low], {"y": ym}),
        (S.at[2, dn], RY.at[1, dn], {"y": ym}),
    )

    def r_send(n):
        src, dst, dev = rspec[n]
        return rcopy(src, dst, rs, rr.at[n], dev)

    def a_send(h):
        at = pl.ds(h * HD, HD)
        return rcopy(AT.at[at], AT2.at[at], ats, atr.at[h], {"xlo": xo})

    def p_send():
        return rcopy(PS, PR, ps, pr, {"xlo": xo})

    def add_into(dst, rows, srcs):
        @pl.loop(0, rows // 64)
        def _(n):
            at = pl.ds(pl.multiple_of(n * 64, 64), 64)
            total = dst[at].astype(F32)
            for src in srcs:
                total = total + src[at].astype(F32)
            dst[at] = total.astype(BF)

    def weight_part(q, rows, j, shift=0, first=0, count=1024):
        @pl.loop(0, count // 256)
        def _(n):
            at = pl.ds(pl.multiple_of(n * 256 + first, 256), 256)
            own_at = pl.ds(pl.multiple_of(n * 256 + shift, 256), 256)
            mine = G[j, :, :, :, :, own_at].reshape(1024, 256)
            pair = G[pair_chunk[q], :, :, :, :, at].reshape(1024, 256)
            S[q, rows, at] = (dot(AT[rows], mine) + dot(AT2[rows], pair)).astype(BF)

    def att_part(acc, j, slot):
        @pl.loop(0, 2)
        def _(a):
            @pl.loop(0, 2)
            def _(b):
                at = pl.ds(pl.multiple_of((a * 2 + b) * 256, 256), 256)
                rows = G[j, a, pl.ds(b * 2, 2)].reshape(256, 1024)
                if isinstance(slot, int):
                    acc[at] += dot(rows, W[slot])
                else:
                    acc[at] += dot(rows[:, :512], W[2, slot]) + dot(rows[:, 512:], W[1, slot])

    def w_start(*which):
        for n in which:
            w_send(n).start()

    def w_wait(*which):
        for n in which:
            w_send(n).wait_recv()

    first = G.at[pl.ds(0, 4), 0, 0, 0]
    pltpu.make_async_copy(first, first, ls.at[0]).wait()
    wcp.wait()
    for d in range(2):
        u_send(0, d, 0).start()
    w_start(0, 1, 2, 3)
    x_send(0).start()
    for d in range(2):
        u_send(5, d, 0).start()
    e_send(0).start()
    e_send(1).start()
    pltpu.make_async_copy(GA, GA, ls.at[2]).wait()
    for h in range(4):
        AT[h * HD : (h + 1) * HD] = GA[h].T
    pltpu.make_async_copy(Q, Q, ls.at[3]).wait()
    for cp in others:
        cp.wait()
    KT[...] = K[...].T
    ACC[...] = jnp.zeros_like(ACC)
    PG[...] = jnp.zeros_like(PG)

    def prob_part(h):
        stat = ST[pl.ds(h, 1)]
        for r in range(4):
            lo = r * 256
            n = 1024 - lo
            scores = dot(K[lo : lo + 256], Q[h, lo:], NT) * scale
            keys_at = lax.broadcasted_iota(jnp.int32, (256, n), 0)
            query_at = lax.broadcasted_iota(jnp.int32, (256, n), 1)
            value = jnp.exp(scores - stat[:, lo:])
            PT[r][h] = jnp.where(keys_at <= query_at, value, 0.0).astype(BF)

    every = pl.ds(0, 512)

    def u_own(j):
        for d in range(2):
            u_send(j, d, 0).start()

    def pump(j):
        x_recv(j).wait_recv()
        u_send(j, 0, 1).start()
        u_send(j, 1, 1).start()
        c_send(j, 0).start()

    def feed(q):
        e_recv(q).wait_recv()
        x_send(q + 1).start()
        u_own(q + 1)

    def relay(j):
        for d in range(2):
            u_recv(j, d).wait_recv()
            z_send(j, d).start()
        c_send(j, 1).start()
        c_send(j, 2).start()

    def land(j):
        z_recv(j).wait_recv()
        c_send(j, 3).start()

    def take(j):
        c_recv(j).wait_recv()

    def a_wait(*which):
        for h in which:
            a_send(h).wait_recv()

    pump(0)
    feed(0)
    e_send(2).start()
    feed(1)
    e_send(3).start()
    prob_part(0)
    relay(0)
    pump(1)
    feed(2)
    w_wait(0, 1)
    w_start(4, 5)
    prob_part(1)
    pump(2)
    feed(3)
    a_send(0).start()
    a_send(1).start()
    x_send(5).start()
    a_send(2).start()
    x_send(6).start()
    a_send(3).start()
    x_send(7).start()
    relay(1)
    land(0)
    prob_part(2)
    pump(3)
    prob_part(3)
    relay(2)
    pump(4)
    land(1)
    take(0)
    w_wait(2, 3, 4, 5)
    att_part(ACC, 0, 3)
    relay(3)
    take(1)
    att_part(PG, 1, 3)
    land(2)
    a_wait(0, 1)
    weight_part(0, up, 0)
    r_send(0).start()
    relay(4)
    u_own(6)
    pump(5)
    u_own(7)
    take(2)
    att_part(PG, 2, 2)
    land(3)
    take(3)
    att_part(PG, 3, 1)
    land(4)
    pump(6)
    take(4)
    att_part(PG, 4, 0)
    PS[...] = PG[...].astype(BF)
    p_send().start()
    relay(5)
    a_wait(2, 3)
    weight_part(0, dn, 0)
    r_send(1).start()
    pump(7)
    land(5)
    relay(6)
    take(5)
    weight_part(1, every, 5, 0, 0, 512)
    r_send(0).wait_recv()
    add_into(S.at[1, up, top], 256, [RH.at[0, :, top]])
    r_send(2).start()
    weight_part(2, every, 5, 512, 0, 512)
    r_send(4).start()
    relay(7)
    land(6)
    att_part(ACC, 5, top)
    take(6)
    weight_part(1, every, 6, 0, 512, 512)
    add_into(S.at[1, up, low], 256, [RH.at[0, :, low]])
    r_send(3).start()
    weight_part(2, every, 6, 512, 512, 512)
    r_send(5).start()
    land(7)
    r_send(1).wait_recv()
    add_into(S.at[2, dn], 256, [RH.at[1]])
    r_send(6).start()
    att_part(ACC, 6, low)
    take(7)
    att_part(ACC, 7, 0)
    weight_part(3, every, 7)
    p_send().wait_recv()
    for h in range(4):
        cols = slice(h * HD, (h + 1) * HD)
        part = (ACC[:, cols] + PR[:, cols].astype(F32)).astype(BF)
        GA[h] = part
        both = part.T.astype(F32) * AT[h * HD : (h + 1) * HD].astype(F32)
        OFF[h : h + 1] = jnp.sum(both, axis=0, keepdims=True)

    zh = lax.rem(z, 2)

    def kv_first(r):
        return rcopy(KB.at[r, :, :, 1 - c], KR1.at[r], ks.at[0], kr.at[0, r], {"core": co})

    def kv_second(r):
        return rcopy(KB2.at[r, 1 - zh], KR2.at[r], ks.at[1], kr.at[1, r], {"z": zpair})

    def kv_middle(r):
        kv_first(r).wait_recv()
        for n in range(2):
            for half in range(2):
                total = KF[r, n, half, c] + KR1[r, n, half].astype(F32)
                KS[r, n, half] = total
                KB2[r, half, n] = total.astype(BF)
        kv_second(r).start()

    for r in range(4):
        lo = r * 256
        mine = slice(lo, lo + 256)
        dv = jnp.zeros((256, HD), F32)
        dk = jnp.zeros((256, HD), F32)
        for h in range(4):
            attention = PT[r][h]
            gb = GA[h, lo:]
            dv = dv + dot(attention, gb)
            grad_att = dot(V[mine], gb, NT)
            grad_scores = (attention.astype(F32) * (grad_att - OFF[h : h + 1, lo:])).astype(BF)
            dk = dk + dot(grad_scores, Q[h, lo:])
            dq = dot(KT[:, mine], grad_scores)
            if r > 0:
                dq = dq + DQ[h, :, lo:]
            DQ[h, :, lo:] = dq
            dq_out[mine, h * HD : (h + 1) * HD] = (dq[:, :256] * scale).T.astype(BF)
        for n, full in enumerate(((dk * scale).T, dv.T)):
            for half in range(2):
                for core in range(2):
                    at = half * 64 + core * 32
                    KF[r, n, half, core] = full[at : at + 32]
                    KB[r, n, half, core] = full[at : at + 32].astype(BF)
        kv_first(r).start()
        if r > 0:
            kv_middle(r - 1)
    kv_middle(3)
    for r in range(4):
        kv_second(r).wait_recv()
        for n in range(2):
            total = KS[r, n, zh] + KR2[r, n].astype(F32)
            (dk_out, dv_out)[n][:, r * 256 : r * 256 + 256] = total.astype(BF)

    r_send(2).wait_recv()
    r_send(3).wait_recv()
    for n in range(4):
        at = slice(n * HD, (n + 1) * HD)
        ACC[:, at] = (S[3, at].astype(F32) + RY[0, at].astype(F32)).T
    for n in range(4):
        at = slice(n * HD, (n + 1) * HD)
        if n == 0:
            r_send(4).wait_recv()
            r_send(5).wait_recv()
        if n == 2:
            r_send(6).wait_recv()
        wg_out[:, at] = (ACC[:, at] + RY[1, at].T.astype(F32)).astype(BF)

    for ref, sem in (
        (first, es),
        (G.at[:, 0, 0, 0], xs),
        (G.at[pl.ds(0, 2)], us),
        (G.at[0], zs),
        (G.at[pl.ds(0, 4)], cs),
        (W.at[pl.ds(0, 3)], ws),
        (S.at[pl.ds(0, 3)], rs),
        (AT, ats),
        (PS, ps),
        (KR1, ks.at[0]),
        (KR2, ks.at[1]),
    ):
        rcopy(ref, ref, sem, sem, {"core": co}).wait_send()


def finish(*refs):
    sems = refs[8]
    copies = [pltpu.make_async_copy(refs[n], refs[4 + n], sems.at[n]) for n in range(4)]
    for cp in copies:
        cp.start()
    for cp in copies:
        cp.wait()


def per_device(grad_out, out_weight, query, keys, values, attended, stats):
    any_spec = pl.BlockSpec(memory_space=pl.ANY)
    vmem = pl.BlockSpec(memory_space=pltpu.VMEM)
    V_ = pltpu.VMEM
    dma = pltpu.SemaphoreType.DMA
    scratch = [
        V_((8, 2, 4, 2, 64, 1024), BF),
        V_((4, 1024, 512), BF),
        V_((4, 512, 1024), BF),
        V_((2, 256, 1024), BF),
        V_((2, 512, 1024), BF),
        V_((512, 1024), BF),
        V_((512, 1024), BF),
        V_((1024, 512), F32),
        V_((1024, 512), F32),
        V_((1024, 512), BF),
        V_((1024, 512), BF),
        V_((4, 1024, HD), BF),
        V_((4, 1024, HD), BF),
        V_((4, 1024), F32),
        V_((1024, HD), BF),
        V_((1024, HD), BF),
        V_((HD, 1024), BF),
        V_((4, 1024), F32),
        V_((4, 256, 1024), BF),
        V_((4, 256, 768), BF),
        V_((4, 256, 512), BF),
        V_((4, 256, 256), BF),
        V_((4, HD, 1024), F32),
        V_((4, 2, 2, 2, 32, 256), F32),
        V_((4, 2, 2, 2, 32, 256), BF),
        V_((4, 2, 2, 32, 256), F32),
        V_((4, 2, 2, 32, 256), BF),
        V_((4, 2, 2, 32, 256), BF),
        V_((4, 2, 32, 256), BF),
        dma, dma((8,)),
        dma, dma((4,)),
        dma, dma((8, 2)),
        dma, dma((8,)),
        dma, dma((8,)),
        dma, dma((6,)),
        dma, dma((7,)),
        dma, dma((4,)),
        dma, dma,
        dma((2,)), dma((2, 4)),
        dma((7,)),
    ]
    dq, dk, dv, wg = pl.pallas_call(
        kernel,
        out_shape=(
            V_((1024, 512), BF),
            V_((32, 1024), BF),
            V_((32, 1024), BF),
            V_((1024, 512), BF),
        ),
        in_specs=[any_spec] * 7,
        out_specs=(vmem,) * 4,
        scratch_shapes=scratch,
        compiler_params=pltpu.CompilerParams(
            collective_id=0, has_side_effects=True, vmem_limit_bytes=58_700_000
        ),
    )(grad_out, out_weight, query, keys, values, attended, stats)
    results = (dq, dk, dv, wg)
    dq, dk, dv, wg = pl.pallas_call(
        finish,
        out_shape=tuple(jax.ShapeDtypeStruct(r.shape, r.dtype) for r in results),
        in_specs=[any_spec] * 4,
        out_specs=(any_spec,) * 4,
        scratch_shapes=[dma((4,))],
        compiler_params=pltpu.CompilerParams(vmem_limit_bytes=1 << 20),
    )(*results)
    return (dq, dk.T, dv.T, wg)


def solution(mesh):
    torus = Mesh(mesh.devices.reshape(4, 2, 2, 4, 2), AXES)
    dp, tp = ("y", "xlo"), ("xhi", "z", "core")
    in_specs = (
        P(dp + tp, None),
        P(dp, tp),
        P(dp, tp),
        P(dp, None),
        P(dp, None),
        P(dp, tp),
        P(tp, dp),
    )
    out_specs = (P(dp, tp), P(dp, tp), P(dp, tp), P(dp, tp))
    return jax.shard_map(
        per_device, mesh=torus, in_specs=in_specs, out_specs=out_specs, check_vma=False
    )
```

```python
import jax
import jax.numpy as jnp
from jax import lax
from jax.experimental import pallas as pl
from jax.experimental.pallas import tpu as pltpu
from jax.sharding import Mesh
from jax.sharding import PartitionSpec as P

HD = 128
GROUP = 16
BF = jnp.bfloat16
F32 = jnp.float32
AXES = ("y", "xlo", "xhi", "z", "core")
NN = (((1,), (0,)), ((), ()))
NT = (((1,), (1,)), ((), ()))


def dot(a, b, dims=NN):
    return lax.dot_general(a, b, dims, preferred_element_type=F32)


def rcopy(src, dst, send, recv, dev):
    return pltpu.make_async_remote_copy(
        src_ref=src,
        dst_ref=dst,
        send_sem=send,
        recv_sem=recv,
        device_id=dev,
        device_id_type=pl.DeviceIdType.MESH,
    )


def kernel(
    g_in, w_in, q_in, k_in, v_in, a_in, st_in,
    dq_out, dk_out, dv_out, wg_out,
    G, W, S, RH, RY, AT, AT2, WT, ACC, PG, PS, PR, Q, GA, K, V, KT, ST,
    P0, P1, P2, P3, DQ, DK, DV, KF, KB, KS, KR1, KB2, KR2,
    xs, xr, es, er, us, ur, zs, zr, cs, cr, ws, wr, rs, rr, ats, atr, ps, pr, ks, kr, ls,
):
    y, xlo, xhi = lax.axis_index("y"), lax.axis_index("xlo"), lax.axis_index("xhi")
    z, c = lax.axis_index("z"), lax.axis_index("core")
    scale = HD ** (-0.5)
    PT = (P0, P1, P2, P3)
    yp, ym, y2 = lax.rem(y + 1, 4), lax.rem(y + 3, 4), lax.rem(y + 2, 4)
    zp, zm, z2 = lax.rem(z + 1, 4), lax.rem(z + 3, 4), lax.rem(z + 2, 4)
    xo, xh, co = 1 - xlo, 1 - xhi, 1 - c
    zpair = z + 1 - 2 * lax.rem(z, 2)

    head = xhi * 2 + z // 2
    hcol = pl.ds(pl.multiple_of(head * HD, HD), HD)
    blocks = (y2, yp, ym, y)
    pair_chunk = (1, 2, 3, 4)

    def columns(q, x, first=0, count=1024):
        return pl.ds(pl.multiple_of((blocks[q] * 2 + x) * 1024 + first, 512), count)

    for q, j in ((0, 0), (3, 7)):
        pltpu.make_async_copy(
            g_in.at[:, columns(q, xlo)], G.at[j, xhi, z, c], ls.at[0]
        ).start()
    for q in (1, 2):
        for half in range(2):
            at = pl.ds((q - 1) * 512, 512)
            pltpu.make_async_copy(
                g_in.at[:, columns(q, xlo, half * 512, 512)],
                G.at[5 + half, xhi, z, c, :, at],
                ls.at[0],
            ).start()
    wcp = pltpu.make_async_copy(w_in, W.at[0], ls.at[1])
    wcp.start()
    for h in range(4):
        pltpu.make_async_copy(a_in.at[:, h * HD : (h + 1) * HD], GA.at[h], ls.at[2]).start()
        pltpu.make_async_copy(q_in.at[:, h * HD : (h + 1) * HD], Q.at[h], ls.at[3]).start()
    others = [
        pltpu.make_async_copy(k_in.at[:, hcol], K, ls.at[4]),
        pltpu.make_async_copy(v_in.at[:, hcol], V, ls.at[5]),
        pltpu.make_async_copy(st_in, ST, ls.at[6]),
    ]
    for cp in others:
        cp.start()

    barrier = pltpu.get_barrier_semaphore()
    for dev in (
        {"y": yp}, {"y": ym}, {"z": zp}, {"z": zm}, {"core": co},
        {"xlo": xo}, {"xhi": xh}, {"xlo": xo, "xhi": xh},
    ):
        pl.semaphore_signal(barrier, inc=1, device_id=dev, device_id_type=pl.DeviceIdType.MESH)
    pl.semaphore_wait(barrier, 8)

    def e_send(q, other):
        dst = G.at[pair_chunk[q], xhi, z, c]
        dev = {"xlo": xo, "xhi": xh} if other else {"xlo": xo}
        return rcopy(g_in.at[:, columns(q, xo)], dst, es, er.at[q, other], dev)

    def e_recv(q, other):
        dst = G.at[pair_chunk[q], (xhi, xh)[other], z, c]
        return rcopy(dst, dst, es, er.at[q, other], {"xlo": xo})

    def x_send(j):
        return rcopy(G.at[j, xhi, z, c], G.at[j, xhi, z, c], xs, xr.at[j], {"xhi": xh})

    def x_recv(j):
        return rcopy(G.at[j, xh, z, c], G.at[j, xh, z, c], xs, xr.at[j], {"xhi": xh})

    def unit(j, zz, cc):
        return G.at[j, :, zz, cc]

    def u_send(j, d, p):
        at = G.at[j, (xhi, xh)[p], z, c]
        return rcopy(at, at, us, ur.at[j, d], {"z": (zp, zm)[d]})

    def u_recv(j, d):
        at = unit(j, (zm, zp)[d], c)
        return rcopy(at, at, us, ur.at[j, d], {"z": (zp, zm)[d]})

    def z_send(j, d):
        at = G.at[j, d, (zm, zp)[d], c]
        return rcopy(at, at, zs, zr.at[j], {"z": (zp, zm)[d]})

    def z_recv(j):
        at = unit(j, z2, c)
        return rcopy(at, at, zs, zr.at[j], {"z": zp})

    slots = (z, zm, zp, z2)

    def c_send(j, s):
        at = unit(j, slots[s], c)
        return rcopy(at, at, cs, cr.at[j], {"core": co})

    def c_recv(j):
        at = G.at[j, :, :, co]
        return rcopy(at, at, cs, cr.at[j], {"core": co})

    top, low = pl.ds(0, 512), pl.ds(512, 512)
    wspec = (
        (W.at[0, top], W.at[1, top], {"y": yp}),
        (W.at[0, low], W.at[2, low], {"y": ym}),
        (W.at[0, low], W.at[1, low], {"y": yp}),
        (W.at[0, top], W.at[2, top], {"y": ym}),
        (W.at[1, top], W.at[3, top], {"y": yp}),
        (W.at[2, low], W.at[3, low], {"y": ym}),
    )

    def w_send(n):
        src, dst, dev = wspec[n]
        return rcopy(src, dst, ws, wr.at[n], dev)

    up, dn = pl.ds(0, 256), pl.ds(256, 256)
    rspec = (
        (S.at[0, up], RH.at[0], {"y": yp}),
        (S.at[0, dn], RH.at[1], {"y": ym}),
        (S.at[1, :, top], RY.at[0, :, top], {"y": yp}),
        (S.at[1, :, low], RY.at[0, :, low], {"y": yp}),
        (S.at[2, :, top], RY.at[1, :, top], {"y": ym}),
        (S.at[2, :, low], RY.at[1, :, low], {"y": ym}),
    )

    def r_send(n):
        src, dst, dev = rspec[n]
        return rcopy(src, dst, rs, rr.at[n], dev)

    def a_send(h):
        at = pl.ds(h * HD, HD)
        return rcopy(AT.at[at], AT2.at[at], ats, atr.at[h], {"xlo": xo})

    def p_send(h):
        return rcopy(PS.at[h], PR.at[h], ps, pr.at[h], {"xlo": xo})

    def add_into(dst, rows, srcs):
        @pl.loop(0, rows // 64)
        def _(n):
            at = pl.ds(pl.multiple_of(n * 64, 64), 64)
            total = dst[at].astype(F32)
            for src in srcs:
                total = total + src[at].astype(F32)
            dst[at] = total.astype(BF)

    def columns_of(j, at):
        return G[j, :, :, :, :, at].reshape(1024, 256)

    def tile(n, first=0):
        return pl.ds(pl.multiple_of(n * 256 + first, 256), 256)

    def weight_part(rows):
        @pl.loop(0, 4)
        def _(n):
            at = tile(n)
            total = dot(AT[rows], columns_of(0, at)) + dot(AT2[rows], columns_of(1, at))
            S[0, rows, at] = total.astype(BF)

    def pair_part(q):
        @pl.loop(0, 4)
        def _(n):
            at = tile(n)
            WT[q - 1, :, at] = dot(AT2[...], columns_of(pair_chunk[q], at))

    def own_part(q, j, shift, first, count):
        @pl.loop(0, count // 256)
        def _(n):
            at = tile(n, first)
            total = WT[q - 1, :, at] + dot(AT[...], columns_of(j, tile(n, shift)))
            S[q, :, at] = total.astype(BF)

    def att_part(acc, j, slot):
        @pl.loop(0, 2)
        def _(a):
            at = pl.ds(pl.multiple_of(a * 512, 512), 512)
            rows = G[j, a].reshape(512, 1024)
            if isinstance(slot, int):
                acc[at] += dot(rows, W[slot])
            else:
                acc[at] += dot(rows[:, :512], W[2, slot]) + dot(rows[:, 512:], W[1, slot])

    def w_start(*which):
        for n in which:
            w_send(n).start()

    def w_wait(*which):
        for n in which:
            w_send(n).wait_recv()

    first = G.at[pl.ds(0, 4), 0, 0, 0]
    pltpu.make_async_copy(first, first, ls.at[0]).wait()
    wcp.wait()
    for d in range(2):
        u_send(0, d, 0).start()
    w_start(0, 1, 2, 3)
    x_send(0).start()
    for d in range(2):
        u_send(5, d, 0).start()
    for q in range(4):
        for other in range(2):
            e_send(q, other).start()
    pltpu.make_async_copy(GA, GA, ls.at[2]).wait()
    for h in range(4):
        AT[h * HD : (h + 1) * HD] = GA[h].T
    pltpu.make_async_copy(Q, Q, ls.at[3]).wait()
    for cp in others:
        cp.wait()
    KT[...] = K[...].T
    ACC[...] = jnp.zeros_like(ACC)
    PG[...] = jnp.zeros_like(PG)

    def prob_part(h):
        stat = ST[pl.ds(h, 1)]
        for r in range(4):
            lo = r * 256
            n = 1024 - lo
            scores = dot(K[lo : lo + 256], Q[h, lo:], NT) * scale
            keys_at = lax.broadcasted_iota(jnp.int32, (256, n), 0)
            query_at = lax.broadcasted_iota(jnp.int32, (256, n), 1)
            value = jnp.exp(scores - stat[:, lo:])
            PT[r][h] = jnp.where(keys_at <= query_at, value, 0.0).astype(BF)

    def u_own(j):
        for d in range(2):
            u_send(j, d, 0).start()

    def pump(j):
        if j in pair_chunk:
            e_recv(j - 1, 1).wait_recv()
        else:
            x_recv(j).wait_recv()
        u_send(j, 0, 1).start()
        u_send(j, 1, 1).start()
        c_send(j, 0).start()

    def feed(q):
        e_recv(q, 0).wait_recv()
        u_own(q + 1)

    def relay(j):
        for d in range(2):
            u_recv(j, d).wait_recv()
            z_send(j, d).start()
        c_send(j, 1).start()
        c_send(j, 2).start()

    def land(j):
        z_recv(j).wait_recv()
        c_send(j, 3).start()

    def take(j):
        c_recv(j).wait_recv()

    def a_wait(*which):
        for h in which:
            a_send(h).wait_recv()

    for h in range(4):
        a_send(h).start()
    for j in (5, 6, 7):
        x_send(j).start()
    pump(0)
    feed(0)
    pump(1)
    prob_part(0)
    relay(0)
    feed(1)
    pump(2)
    w_wait(0, 1)
    w_start(4, 5)
    prob_part(1)
    relay(1)
    feed(2)
    pump(3)
    prob_part(2)
    land(0)
    prob_part(3)
    relay(2)
    feed(3)
    pump(4)
    land(1)
    take(0)
    take(1)
    a_wait(0, 1)
    weight_part(up)
    r_send(0).start()
    relay(3)
    w_wait(2, 3, 4, 5)
    att_part(ACC, 0, 3)
    land(2)
    att_part(PG, 1, 3)
    take(2)
    a_wait(2, 3)
    weight_part(dn)
    r_send(1).start()
    relay(4)
    pump(5)
    u_own(6)
    att_part(PG, 2, 2)
    land(3)
    take(3)
    att_part(PG, 3, 1)
    land(4)
    relay(5)
    pump(6)
    u_own(7)
    pump(7)
    take(4)
    att_part(PG, 4, 0)
    for h in range(4):
        PS[h] = PG[:, h * HD : (h + 1) * HD].astype(BF)
        p_send(h).start()
    pair_part(1)
    land(5)
    pair_part(2)
    take(5)
    own_part(1, 5, 0, 0, 512)
    r_send(0).wait_recv()
    add_into(S.at[1, up, top], 256, [RH.at[0, :, top]])
    r_send(2).start()
    relay(6)
    own_part(2, 5, 512, 0, 512)
    r_send(1).wait_recv()
    add_into(S.at[2, dn, top], 256, [RH.at[1, :, top]])
    r_send(4).start()
    pair_part(3)
    att_part(ACC, 5, top)
    relay(7)
    land(6)
    take(6)
    own_part(1, 6, 0, 512, 512)
    add_into(S.at[1, up, low], 256, [RH.at[0, :, low]])
    r_send(3).start()
    own_part(2, 6, 512, 512, 512)
    add_into(S.at[2, dn, low], 256, [RH.at[1, :, low]])
    r_send(5).start()
    land(7)
    att_part(ACC, 6, low)
    take(7)
    att_part(ACC, 7, 0)

    zh = lax.rem(z, 2)

    def kv_first(r):
        return rcopy(KB.at[r, :, :, 1 - c], KR1.at[r], ks.at[0], kr.at[0, r], {"core": co})

    def kv_second(r):
        return rcopy(KB2.at[r, 1 - zh], KR2.at[r], ks.at[1], kr.at[1, r], {"z": zpair})

    def kv_middle(r):
        kv_first(r).wait_recv()
        for n in range(2):
            for half in range(2):
                total = KF[r, n, half, c] + KR1[r, n, half].astype(F32)
                KS[r, n, half] = total
                KB2[r, half, n] = total.astype(BF)
        kv_second(r).start()

    for h in range(4):
        cols = slice(h * HD, (h + 1) * HD)
        p_send(h).wait_recv()
        part = (ACC[:, cols] + PR[h].astype(F32)).astype(BF)
        GA[h] = part
        offset = jnp.sum(part.T.astype(F32) * AT[cols].astype(F32), axis=0, keepdims=True)
        for r in range(4):
            lo = r * 256
            mine = slice(lo, lo + 256)
            attention = PT[r][h]
            gb = GA[h, lo:]
            dv = dot(attention, gb)
            grad_att = dot(V[mine], gb, NT)
            grad_scores = (attention.astype(F32) * (grad_att - offset[:, lo:])).astype(BF)
            dk = dot(grad_scores, Q[h, lo:])
            dq = dot(KT[:, mine], grad_scores)
            if r > 0:
                dq = dq + DQ[:, lo:]
            DQ[:, lo:] = dq
            dq_out[mine, cols] = (dq[:, :256] * scale).T.astype(BF)
            if h > 0:
                dv = dv + DV[r]
                dk = dk + DK[r]
            if h < 3:
                DV[r] = dv
                DK[r] = dk
                continue
            for n, full in enumerate(((dk * scale).T, dv.T)):
                for half in range(2):
                    for core in range(2):
                        at = half * 64 + core * 32
                        KF[r, n, half, core] = full[at : at + 32]
                        KB[r, n, half, core] = full[at : at + 32].astype(BF)
            kv_first(r).start()
            if r > 0:
                kv_middle(r - 1)
    kv_middle(3)
    for half in range(2):
        r_send(2 + half).wait_recv()
        r_send(4 + half).wait_recv()

        @pl.loop(0, 2)
        def _(n):
            at = tile(n, half * 512)
            total = WT[2, :, at] + dot(AT[...], columns_of(7, at))
            total = total + RY[0, :, at].astype(F32) + RY[1, :, at].astype(F32)
            wg_out[at] = total.T.astype(BF)

    for r in range(4):
        kv_second(r).wait_recv()
        for n in range(2):
            total = KS[r, n, zh] + KR2[r, n].astype(F32)
            (dk_out, dv_out)[n][:, r * 256 : r * 256 + 256] = total.astype(BF)

    for ref, sem in (
        (G.at[:, 0, 0, 0], es),
        (first, xs),
        (G.at[pl.ds(0, 2)], us),
        (G.at[0], zs),
        (G.at[pl.ds(0, 4)], cs),
        (W.at[pl.ds(0, 3)], ws),
        (S, rs),
        (AT, ats),
        (PS, ps),
        (KR1, ks.at[0]),
        (KR2, ks.at[1]),
    ):
        rcopy(ref, ref, sem, sem, {"core": co}).wait_send()


def finish(*refs):
    sems = refs[8]
    copies = [pltpu.make_async_copy(refs[n], refs[4 + n], sems.at[n]) for n in range(4)]
    for cp in copies:
        cp.start()
    for cp in copies:
        cp.wait()


def per_device(grad_out, out_weight, query, keys, values, attended, stats):
    any_spec = pl.BlockSpec(memory_space=pl.ANY)
    vmem = pl.BlockSpec(memory_space=pltpu.VMEM)
    V_ = pltpu.VMEM
    dma = pltpu.SemaphoreType.DMA
    scratch = [
        V_((8, 2, 4, 2, 64, 1024), BF),
        V_((4, 1024, 512), BF),
        V_((3, 512, 1024), BF),
        V_((2, 256, 1024), BF),
        V_((2, 512, 1024), BF),
        V_((512, 1024), BF),
        V_((512, 1024), BF),
        V_((3, 512, 1024), F32),
        V_((1024, 512), F32),
        V_((1024, 512), F32),
        V_((4, 1024, HD), BF),
        V_((4, 1024, HD), BF),
        V_((4, 1024, HD), BF),
        V_((4, 1024, HD), BF),
        V_((1024, HD), BF),
        V_((1024, HD), BF),
        V_((HD, 1024), BF),
        V_((4, 1024), F32),
        V_((4, 256, 1024), BF),
        V_((4, 256, 768), BF),
        V_((4, 256, 512), BF),
        V_((4, 256, 256), BF),
        V_((HD, 1024), F32),
        V_((4, 256, HD), F32),
        V_((4, 256, HD), F32),
        V_((4, 2, 2, 2, 32, 256), F32),
        V_((4, 2, 2, 2, 32, 256), BF),
        V_((4, 2, 2, 32, 256), F32),
        V_((4, 2, 2, 32, 256), BF),
        V_((4, 2, 2, 32, 256), BF),
        V_((4, 2, 32, 256), BF),
        dma, dma((8,)),
        dma, dma((4, 2)),
        dma, dma((8, 2)),
        dma, dma((8,)),
        dma, dma((8,)),
        dma, dma((6,)),
        dma, dma((6,)),
        dma, dma((4,)),
        dma, dma((4,)),
        dma((2,)), dma((2, 4)),
        dma((7,)),
    ]
    dq, dk, dv, wg = pl.pallas_call(
        kernel,
        out_shape=(
            V_((1024, 512), BF),
            V_((32, 1024), BF),
            V_((32, 1024), BF),
            V_((1024, 512), BF),
        ),
        in_specs=[any_spec] * 7,
        out_specs=(vmem,) * 4,
        scratch_shapes=scratch,
        compiler_params=pltpu.CompilerParams(
            collective_id=0, has_side_effects=True, vmem_limit_bytes=58_700_000
        ),
    )(grad_out, out_weight, query, keys, values, attended, stats)
    results = (dq, dk, dv, wg)
    dq, dk, dv, wg = pl.pallas_call(
        finish,
        out_shape=tuple(jax.ShapeDtypeStruct(r.shape, r.dtype) for r in results),
        in_specs=[any_spec] * 4,
        out_specs=(any_spec,) * 4,
        scratch_shapes=[dma((4,))],
        compiler_params=pltpu.CompilerParams(vmem_limit_bytes=1 << 20),
    )(*results)
    return (dq, dk.T, dv.T, wg)


def solution(mesh):
    torus = Mesh(mesh.devices.reshape(4, 2, 2, 4, 2), AXES)
    dp, tp = ("y", "xlo"), ("xhi", "z", "core")
    in_specs = (
        P(dp + tp, None),
        P(dp, tp),
        P(dp, tp),
        P(dp, None),
        P(dp, None),
        P(dp, tp),
        P(tp, dp),
    )
    out_specs = (P(dp, tp), P(dp, tp), P(dp, tp), P(dp, tp))
    return jax.shard_map(
        per_device, mesh=torus, in_specs=in_specs, out_specs=out_specs, check_vma=False
    )
```

```python
import jax
import jax.numpy as jnp
from jax import lax
from jax.experimental import pallas as pl
from jax.experimental.pallas import tpu as pltpu
from jax.sharding import Mesh
from jax.sharding import PartitionSpec as P

HD = 128
GROUP = 16
BF = jnp.bfloat16
F32 = jnp.float32
AXES = ("y", "xlo", "xhi", "z", "core")
NN = (((1,), (0,)), ((), ()))
NT = (((1,), (1,)), ((), ()))


def dot(a, b, dims=NN):
    return lax.dot_general(a, b, dims, preferred_element_type=F32)


def rcopy(src, dst, send, recv, dev):
    return pltpu.make_async_remote_copy(
        src_ref=src,
        dst_ref=dst,
        send_sem=send,
        recv_sem=recv,
        device_id=dev,
        device_id_type=pl.DeviceIdType.MESH,
    )


def kernel(
    g_in, w_in, q_in, k_in, v_in, a_in, st_in,
    dq_out, dk_out, dv_out, wg_out,
    G, W, S, RH, RY, AT, AT2, WT, ACC, PG, PS, PR, Q, GA, K, V, KT, ST,
    P0, P1, P2, P3, DQ, DK, DV, KF, KB, KS, KR1, KB2, KR2,
    xs, xr, es, er, us, ur, zs, zr, cs, cr, ws, wr, rs, rr, ats, atr, ps, pr, ks, kr, ls,
):
    y, xlo, xhi = lax.axis_index("y"), lax.axis_index("xlo"), lax.axis_index("xhi")
    z, c = lax.axis_index("z"), lax.axis_index("core")
    scale = HD ** (-0.5)
    PT = (P0, P1, P2, P3)
    yp, ym, y2 = lax.rem(y + 1, 4), lax.rem(y + 3, 4), lax.rem(y + 2, 4)
    zp, zm, z2 = lax.rem(z + 1, 4), lax.rem(z + 3, 4), lax.rem(z + 2, 4)
    xo, xh, co = 1 - xlo, 1 - xhi, 1 - c
    zpair = z + 1 - 2 * lax.rem(z, 2)

    head = xhi * 2 + z // 2
    hcol = pl.ds(pl.multiple_of(head * HD, HD), HD)
    blocks = (y2, yp, ym, y)
    pair_chunk = (1, 2, 3, 4)

    def columns(q, x, first=0, count=1024):
        return pl.ds(pl.multiple_of((blocks[q] * 2 + x) * 1024 + first, 512), count)

    for q, j in ((0, 0), (3, 7)):
        pltpu.make_async_copy(
            g_in.at[:, columns(q, xlo)], G.at[j, xhi, z, c], ls.at[0]
        ).start()
    for q in (1, 2):
        for half in range(2):
            at = pl.ds((q - 1) * 512, 512)
            pltpu.make_async_copy(
                g_in.at[:, columns(q, xlo, half * 512, 512)],
                G.at[5 + half, xhi, z, c, :, at],
                ls.at[0],
            ).start()
    wcp = pltpu.make_async_copy(w_in, W.at[0], ls.at[1])
    wcp.start()
    for h in range(4):
        pltpu.make_async_copy(a_in.at[:, h * HD : (h + 1) * HD], GA.at[h], ls.at[2]).start()
        pltpu.make_async_copy(q_in.at[:, h * HD : (h + 1) * HD], Q.at[h], ls.at[3]).start()
    others = [
        pltpu.make_async_copy(k_in.at[:, hcol], K, ls.at[4]),
        pltpu.make_async_copy(v_in.at[:, hcol], V, ls.at[5]),
        pltpu.make_async_copy(st_in, ST, ls.at[6]),
    ]
    for cp in others:
        cp.start()

    barrier = pltpu.get_barrier_semaphore()
    for dev in (
        {"y": yp}, {"y": ym}, {"z": zp}, {"z": zm}, {"core": co},
        {"xlo": xo}, {"xhi": xh}, {"xlo": xo, "xhi": xh},
    ):
        pl.semaphore_signal(barrier, inc=1, device_id=dev, device_id_type=pl.DeviceIdType.MESH)
    pl.semaphore_wait(barrier, 8)

    def e_send(q, other):
        dst = G.at[pair_chunk[q], xhi, z, c]
        dev = {"xlo": xo, "xhi": xh} if other else {"xlo": xo}
        return rcopy(g_in.at[:, columns(q, xo)], dst, es, er.at[q, other], dev)

    def e_recv(q, other):
        dst = G.at[pair_chunk[q], (xhi, xh)[other], z, c]
        return rcopy(dst, dst, es, er.at[q, other], {"xlo": xo})

    def x_send(j):
        return rcopy(G.at[j, xhi, z, c], G.at[j, xhi, z, c], xs, xr.at[j], {"xhi": xh})

    def x_recv(j):
        return rcopy(G.at[j, xh, z, c], G.at[j, xh, z, c], xs, xr.at[j], {"xhi": xh})

    def unit(j, zz, cc):
        return G.at[j, :, zz, cc]

    def u_send(j, d, p):
        at = G.at[j, (xhi, xh)[p], z, c]
        return rcopy(at, at, us, ur.at[j, d], {"z": (zp, zm)[d]})

    def u_recv(j, d):
        at = unit(j, (zm, zp)[d], c)
        return rcopy(at, at, us, ur.at[j, d], {"z": (zp, zm)[d]})

    def z_send(j, d):
        at = G.at[j, d, (zm, zp)[d], c]
        return rcopy(at, at, zs, zr.at[j], {"z": (zp, zm)[d]})

    def z_recv(j):
        at = unit(j, z2, c)
        return rcopy(at, at, zs, zr.at[j], {"z": zp})

    slots = (z, zm, zp, z2)

    def c_send(j, s):
        at = unit(j, slots[s], c)
        return rcopy(at, at, cs, cr.at[j], {"core": co})

    def c_recv(j):
        at = G.at[j, :, :, co]
        return rcopy(at, at, cs, cr.at[j], {"core": co})

    top, low = pl.ds(0, 512), pl.ds(512, 512)
    wspec = (
        (W.at[0, top], W.at[1, top], {"y": yp}),
        (W.at[0, low], W.at[2, low], {"y": ym}),
        (W.at[0, low], W.at[1, low], {"y": yp}),
        (W.at[0, top], W.at[2, top], {"y": ym}),
        (W.at[1, top], W.at[3, top], {"y": yp}),
        (W.at[2, low], W.at[3, low], {"y": ym}),
    )

    def w_send(n):
        src, dst, dev = wspec[n]
        return rcopy(src, dst, ws, wr.at[n], dev)

    up, dn = pl.ds(0, 256), pl.ds(256, 256)
    rspec = (
        (S.at[0, up], RH.at[0], {"y": yp}),
        (S.at[0, dn], RH.at[1], {"y": ym}),
        (S.at[1, :, top], RY.at[0, :, top], {"y": yp}),
        (S.at[1, :, low], RY.at[0, :, low], {"y": yp}),
        (S.at[2, :, top], RY.at[1, :, top], {"y": ym}),
        (S.at[2, :, low], RY.at[1, :, low], {"y": ym}),
    )

    def r_send(n):
        src, dst, dev = rspec[n]
        return rcopy(src, dst, rs, rr.at[n], dev)

    def a_send(h):
        at = pl.ds(h * HD, HD)
        return rcopy(AT.at[at], AT2.at[at], ats, atr.at[h], {"xlo": xo})

    def p_send(h):
        return rcopy(PS.at[h], PR.at[h], ps, pr.at[h], {"xlo": xo})

    def add_into(dst, rows, srcs):
        @pl.loop(0, rows // 64)
        def _(n):
            at = pl.ds(pl.multiple_of(n * 64, 64), 64)
            total = dst[at].astype(F32)
            for src in srcs:
                total = total + src[at].astype(F32)
            dst[at] = total.astype(BF)

    def columns_of(j, at):
        return G[j, :, :, :, :, at].reshape(1024, 512)

    def tile(n, first=0):
        return pl.ds(pl.multiple_of(n * 512 + first, 512), 512)

    def weight_part(rows):
        @pl.loop(0, 2)
        def _(n):
            at = tile(n)
            total = dot(AT[rows], columns_of(0, at)) + dot(AT2[rows], columns_of(1, at))
            S[0, rows, at] = total.astype(BF)

    def pair_part(q):
        @pl.loop(0, 2)
        def _(n):
            at = tile(n)
            WT[q - 1, :, at] = dot(AT2[...], columns_of(pair_chunk[q], at))

    def own_part(q, j, shift, first, count):
        @pl.loop(0, count // 512)
        def _(n):
            at = tile(n, first)
            total = WT[q - 1, :, at] + dot(AT[...], columns_of(j, tile(n, shift)))
            S[q, :, at] = total.astype(BF)

    def att_part(acc, j, slot):
        @pl.loop(0, 2)
        def _(a):
            at = pl.ds(pl.multiple_of(a * 512, 512), 512)
            rows = G[j, a].reshape(512, 1024)
            if isinstance(slot, int):
                acc[at] += dot(rows, W[slot])
            else:
                acc[at] += dot(rows[:, :512], W[2, slot]) + dot(rows[:, 512:], W[1, slot])

    def w_start(*which):
        for n in which:
            w_send(n).start()

    def w_wait(*which):
        for n in which:
            w_send(n).wait_recv()

    first = G.at[pl.ds(0, 4), 0, 0, 0]
    pltpu.make_async_copy(first, first, ls.at[0]).wait()
    wcp.wait()
    for d in range(2):
        u_send(0, d, 0).start()
    w_start(0, 1, 2, 3)
    x_send(0).start()
    for d in range(2):
        u_send(5, d, 0).start()
    for q in range(4):
        for other in range(2):
            e_send(q, other).start()
    pltpu.make_async_copy(GA, GA, ls.at[2]).wait()
    for h in range(4):
        AT[h * HD : (h + 1) * HD] = GA[h].T
    pltpu.make_async_copy(Q, Q, ls.at[3]).wait()
    for cp in others:
        cp.wait()
    KT[...] = K[...].T
    ACC[...] = jnp.zeros_like(ACC)
    PG[...] = jnp.zeros_like(PG)

    def prob_part(h):
        stat = ST[pl.ds(h, 1)]
        for r in range(4):
            lo = r * 256
            n = 1024 - lo
            scores = dot(K[lo : lo + 256], Q[h, lo:], NT) * scale
            keys_at = lax.broadcasted_iota(jnp.int32, (256, n), 0)
            query_at = lax.broadcasted_iota(jnp.int32, (256, n), 1)
            value = jnp.exp(scores - stat[:, lo:])
            PT[r][h] = jnp.where(keys_at <= query_at, value, 0.0).astype(BF)

    def u_own(j):
        for d in range(2):
            u_send(j, d, 0).start()

    def pump(j):
        if j in pair_chunk:
            e_recv(j - 1, 1).wait_recv()
        else:
            x_recv(j).wait_recv()
        u_send(j, 0, 1).start()
        u_send(j, 1, 1).start()
        c_send(j, 0).start()

    def feed(q):
        e_recv(q, 0).wait_recv()
        u_own(q + 1)

    def relay(j):
        for d in range(2):
            u_recv(j, d).wait_recv()
            z_send(j, d).start()
        c_send(j, 1).start()
        c_send(j, 2).start()

    def land(j):
        z_recv(j).wait_recv()
        c_send(j, 3).start()

    def take(j):
        c_recv(j).wait_recv()

    def a_wait(*which):
        for h in which:
            a_send(h).wait_recv()

    for h in range(4):
        a_send(h).start()
    for j in (5, 6, 7):
        x_send(j).start()
    pump(0)
    feed(0)
    pump(1)
    prob_part(0)
    relay(0)
    feed(1)
    pump(2)
    w_wait(0, 1)
    w_start(4, 5)
    prob_part(1)
    relay(1)
    feed(2)
    pump(3)
    prob_part(2)
    land(0)
    prob_part(3)
    relay(2)
    feed(3)
    pump(4)
    land(1)
    take(0)
    take(1)
    a_wait(0, 1)
    weight_part(up)
    r_send(0).start()
    relay(3)
    w_wait(2, 3, 4, 5)
    att_part(ACC, 0, 3)
    land(2)
    att_part(PG, 1, 3)
    take(2)
    a_wait(2, 3)
    weight_part(dn)
    r_send(1).start()
    relay(4)
    pump(5)
    u_own(6)
    att_part(PG, 2, 2)
    land(3)
    take(3)
    att_part(PG, 3, 1)
    land(4)
    relay(5)
    pump(6)
    u_own(7)
    pump(7)
    take(4)
    att_part(PG, 4, 0)
    for h in range(4):
        PS[h] = PG[:, h * HD : (h + 1) * HD].astype(BF)
        p_send(h).start()
    pair_part(1)
    land(5)
    pair_part(2)
    take(5)
    own_part(1, 5, 0, 0, 512)
    r_send(0).wait_recv()
    add_into(S.at[1, up, top], 256, [RH.at[0, :, top]])
    r_send(2).start()
    own_part(2, 5, 512, 0, 512)
    r_send(1).wait_recv()
    add_into(S.at[2, dn, top], 256, [RH.at[1, :, top]])
    r_send(4).start()
    relay(6)
    pair_part(3)
    att_part(ACC, 5, top)
    relay(7)
    land(6)
    take(6)
    own_part(1, 6, 0, 512, 512)
    add_into(S.at[1, up, low], 256, [RH.at[0, :, low]])
    r_send(3).start()
    own_part(2, 6, 512, 512, 512)
    add_into(S.at[2, dn, low], 256, [RH.at[1, :, low]])
    r_send(5).start()
    land(7)
    att_part(ACC, 6, low)
    take(7)
    att_part(ACC, 7, 0)

    zh = lax.rem(z, 2)

    def kv_first(r):
        return rcopy(KB.at[r, :, :, 1 - c], KR1.at[r], ks.at[0], kr.at[0, r], {"core": co})

    def kv_second(r):
        return rcopy(KB2.at[r, 1 - zh], KR2.at[r], ks.at[1], kr.at[1, r], {"z": zpair})

    def kv_middle(r):
        kv_first(r).wait_recv()
        for n in range(2):
            for half in range(2):
                total = KF[r, n, half, c] + KR1[r, n, half].astype(F32)
                KS[r, n, half] = total
                KB2[r, half, n] = total.astype(BF)
        kv_second(r).start()

    for h in range(4):
        cols = slice(h * HD, (h + 1) * HD)
        p_send(h).wait_recv()
        part = (ACC[:, cols] + PR[h].astype(F32)).astype(BF)
        GA[h] = part
        offset = jnp.sum(part.T.astype(F32) * AT[cols].astype(F32), axis=0, keepdims=True)
        for r in range(4):
            lo = r * 256
            mine = slice(lo, lo + 256)
            attention = PT[r][h]
            gb = GA[h, lo:]
            dv = dot(attention, gb)
            grad_att = dot(V[mine], gb, NT)
            grad_scores = (attention.astype(F32) * (grad_att - offset[:, lo:])).astype(BF)
            dk = dot(grad_scores, Q[h, lo:])
            dq = dot(KT[:, mine], grad_scores)
            if r > 0:
                dq = dq + DQ[:, lo:]
            DQ[:, lo:] = dq
            dq_out[mine, cols] = (dq[:, :256] * scale).T.astype(BF)
            if h > 0:
                dv = dv + DV[r]
                dk = dk + DK[r]
            if h < 3:
                DV[r] = dv
                DK[r] = dk
                continue
            for n, full in enumerate(((dk * scale).T, dv.T)):
                for half in range(2):
                    for core in range(2):
                        at = half * 64 + core * 32
                        KF[r, n, half, core] = full[at : at + 32]
                        KB[r, n, half, core] = full[at : at + 32].astype(BF)
            kv_first(r).start()
            if r > 0:
                kv_middle(r - 1)
    kv_middle(3)
    for half in range(2):
        r_send(2 + half).wait_recv()
        r_send(4 + half).wait_recv()

        at = tile(half)
        total = WT[2, :, at] + dot(AT[...], columns_of(7, at))
        total = total + RY[0, :, at].astype(F32) + RY[1, :, at].astype(F32)
        wg_out[at] = total.T.astype(BF)

    for r in range(4):
        kv_second(r).wait_recv()
        for n in range(2):
            total = KS[r, n, zh] + KR2[r, n].astype(F32)
            (dk_out, dv_out)[n][:, r * 256 : r * 256 + 256] = total.astype(BF)

    for ref, sem in (
        (G.at[:, 0, 0, 0], es),
        (first, xs),
        (G.at[pl.ds(0, 2)], us),
        (G.at[0], zs),
        (G.at[pl.ds(0, 4)], cs),
        (W.at[pl.ds(0, 3)], ws),
        (S, rs),
        (AT, ats),
        (PS, ps),
        (KR1, ks.at[0]),
        (KR2, ks.at[1]),
    ):
        rcopy(ref, ref, sem, sem, {"core": co}).wait_send()


def finish(*refs):
    sems = refs[8]
    copies = [pltpu.make_async_copy(refs[n], refs[4 + n], sems.at[n]) for n in range(4)]
    for cp in copies:
        cp.start()
    for cp in copies:
        cp.wait()


def per_device(grad_out, out_weight, query, keys, values, attended, stats):
    any_spec = pl.BlockSpec(memory_space=pl.ANY)
    vmem = pl.BlockSpec(memory_space=pltpu.VMEM)
    V_ = pltpu.VMEM
    dma = pltpu.SemaphoreType.DMA
    scratch = [
        V_((8, 2, 4, 2, 64, 1024), BF),
        V_((4, 1024, 512), BF),
        V_((3, 512, 1024), BF),
        V_((2, 256, 1024), BF),
        V_((2, 512, 1024), BF),
        V_((512, 1024), BF),
        V_((512, 1024), BF),
        V_((3, 512, 1024), F32),
        V_((1024, 512), F32),
        V_((1024, 512), F32),
        V_((4, 1024, HD), BF),
        V_((4, 1024, HD), BF),
        V_((4, 1024, HD), BF),
        V_((4, 1024, HD), BF),
        V_((1024, HD), BF),
        V_((1024, HD), BF),
        V_((HD, 1024), BF),
        V_((4, 1024), F32),
        V_((4, 256, 1024), BF),
        V_((4, 256, 768), BF),
        V_((4, 256, 512), BF),
        V_((4, 256, 256), BF),
        V_((HD, 1024), F32),
        V_((4, 256, HD), F32),
        V_((4, 256, HD), F32),
        V_((4, 2, 2, 2, 32, 256), F32),
        V_((4, 2, 2, 2, 32, 256), BF),
        V_((4, 2, 2, 32, 256), F32),
        V_((4, 2, 2, 32, 256), BF),
        V_((4, 2, 2, 32, 256), BF),
        V_((4, 2, 32, 256), BF),
        dma, dma((8,)),
        dma, dma((4, 2)),
        dma, dma((8, 2)),
        dma, dma((8,)),
        dma, dma((8,)),
        dma, dma((6,)),
        dma, dma((6,)),
        dma, dma((4,)),
        dma, dma((4,)),
        dma((2,)), dma((2, 4)),
        dma((7,)),
    ]
    dq, dk, dv, wg = pl.pallas_call(
        kernel,
        out_shape=(
            V_((1024, 512), BF),
            V_((32, 1024), BF),
            V_((32, 1024), BF),
            V_((1024, 512), BF),
        ),
        in_specs=[any_spec] * 7,
        out_specs=(vmem,) * 4,
        scratch_shapes=scratch,
        compiler_params=pltpu.CompilerParams(
            collective_id=0, has_side_effects=True, vmem_limit_bytes=58_700_000
        ),
    )(grad_out, out_weight, query, keys, values, attended, stats)
    results = (dq, dk, dv, wg)
    dq, dk, dv, wg = pl.pallas_call(
        finish,
        out_shape=tuple(jax.ShapeDtypeStruct(r.shape, r.dtype) for r in results),
        in_specs=[any_spec] * 4,
        out_specs=(any_spec,) * 4,
        scratch_shapes=[dma((4,))],
        compiler_params=pltpu.CompilerParams(vmem_limit_bytes=1 << 20),
    )(*results)
    return (dq, dk.T, dv.T, wg)


def solution(mesh):
    torus = Mesh(mesh.devices.reshape(4, 2, 2, 4, 2), AXES)
    dp, tp = ("y", "xlo"), ("xhi", "z", "core")
    in_specs = (
        P(dp + tp, None),
        P(dp, tp),
        P(dp, tp),
        P(dp, None),
        P(dp, None),
        P(dp, tp),
        P(tp, dp),
    )
    out_specs = (P(dp, tp), P(dp, tp), P(dp, tp), P(dp, tp))
    return jax.shard_map(
        per_device, mesh=torus, in_specs=in_specs, out_specs=out_specs, check_vma=False
    )
```

```python
import jax
import jax.numpy as jnp
from jax import lax
from jax.experimental import pallas as pl
from jax.experimental.pallas import tpu as pltpu
from jax.sharding import Mesh
from jax.sharding import PartitionSpec as P

HD = 128
GROUP = 16
BF = jnp.bfloat16
F32 = jnp.float32
AXES = ("y", "xlo", "xhi", "z", "core")
NN = (((1,), (0,)), ((), ()))
NT = (((1,), (1,)), ((), ()))


def dot(a, b, dims=NN):
    return lax.dot_general(a, b, dims, preferred_element_type=F32)


def rcopy(src, dst, send, recv, dev):
    return pltpu.make_async_remote_copy(
        src_ref=src,
        dst_ref=dst,
        send_sem=send,
        recv_sem=recv,
        device_id=dev,
        device_id_type=pl.DeviceIdType.MESH,
    )


def kernel(
    g_in, w_in, q_in, k_in, v_in, a_in, st_in,
    dq_out, dk_out, dv_out, wg_out,
    G, W, S, RH, RY, AT, AT2, WT, ACC, PG, PS, PR, Q, GA, K, V, KT, ST,
    P0, P1, P2, P3, DQ, DK, DV, KF, KB, KS, KR1, KB2, KR2,
    xs, xr, es, er, us, ur, zs, zr, cs, cr, ws, wr, rs, rr, ats, atr, ps, pr, ks, kr, ls,
):
    y, xlo, xhi = lax.axis_index("y"), lax.axis_index("xlo"), lax.axis_index("xhi")
    z, c = lax.axis_index("z"), lax.axis_index("core")
    scale = HD ** (-0.5)
    PT = (P0, P1, P2, P3)
    yp, ym, y2 = lax.rem(y + 1, 4), lax.rem(y + 3, 4), lax.rem(y + 2, 4)
    zp, zm, z2 = lax.rem(z + 1, 4), lax.rem(z + 3, 4), lax.rem(z + 2, 4)
    xo, xh, co = 1 - xlo, 1 - xhi, 1 - c
    zpair = z + 1 - 2 * lax.rem(z, 2)

    head = xhi * 2 + z // 2
    hcol = pl.ds(pl.multiple_of(head * HD, HD), HD)
    blocks = (y2, yp, ym, y)
    pair_chunk = (1, 2, 3, 4)

    def columns(q, x, first=0, count=1024):
        return pl.ds(pl.multiple_of((blocks[q] * 2 + x) * 1024 + first, 512), count)

    for q, j in ((0, 0), (3, 7)):
        pltpu.make_async_copy(
            g_in.at[:, columns(q, xlo)], G.at[j, xhi, z, c], ls.at[0]
        ).start()
    for q in (1, 2):
        for half in range(2):
            at = pl.ds((q - 1) * 512, 512)
            pltpu.make_async_copy(
                g_in.at[:, columns(q, xlo, half * 512, 512)],
                G.at[5 + half, xhi, z, c, :, at],
                ls.at[0],
            ).start()
    wcp = pltpu.make_async_copy(w_in, W.at[0], ls.at[1])
    wcp.start()
    for h in range(4):
        pltpu.make_async_copy(a_in.at[:, h * HD : (h + 1) * HD], GA.at[h], ls.at[2]).start()
        pltpu.make_async_copy(q_in.at[:, h * HD : (h + 1) * HD], Q.at[h], ls.at[3]).start()
    others = [
        pltpu.make_async_copy(k_in.at[:, hcol], K, ls.at[4]),
        pltpu.make_async_copy(v_in.at[:, hcol], V, ls.at[5]),
        pltpu.make_async_copy(st_in, ST, ls.at[6]),
    ]
    for cp in others:
        cp.start()

    barrier = pltpu.get_barrier_semaphore()
    for dev in (
        {"y": yp}, {"y": ym}, {"z": zp}, {"z": zm}, {"core": co},
        {"xlo": xo}, {"xhi": xh}, {"xlo": xo, "xhi": xh},
    ):
        pl.semaphore_signal(barrier, inc=1, device_id=dev, device_id_type=pl.DeviceIdType.MESH)
    pl.semaphore_wait(barrier, 8)

    def e_send(q, other):
        dst = G.at[pair_chunk[q], xhi, z, c]
        dev = {"xlo": xo, "xhi": xh} if other else {"xlo": xo}
        return rcopy(g_in.at[:, columns(q, xo)], dst, es, er.at[q, other], dev)

    def e_recv(q, other):
        dst = G.at[pair_chunk[q], (xhi, xh)[other], z, c]
        return rcopy(dst, dst, es, er.at[q, other], {"xlo": xo})

    def x_send(j):
        return rcopy(G.at[j, xhi, z, c], G.at[j, xhi, z, c], xs, xr.at[j], {"xhi": xh})

    def x_recv(j):
        return rcopy(G.at[j, xh, z, c], G.at[j, xh, z, c], xs, xr.at[j], {"xhi": xh})

    def unit(j, zz, cc):
        return G.at[j, :, zz, cc]

    def u_send(j, d, p):
        at = G.at[j, (xhi, xh)[p], z, c]
        return rcopy(at, at, us, ur.at[j, d], {"z": (zp, zm)[d]})

    def u_recv(j, d):
        at = unit(j, (zm, zp)[d], c)
        return rcopy(at, at, us, ur.at[j, d], {"z": (zp, zm)[d]})

    def z_send(j, d):
        at = G.at[j, d, (zm, zp)[d], c]
        return rcopy(at, at, zs, zr.at[j], {"z": (zp, zm)[d]})

    def z_recv(j):
        at = unit(j, z2, c)
        return rcopy(at, at, zs, zr.at[j], {"z": zp})

    slots = (z, zm, zp, z2)

    def c_send(j, s):
        at = unit(j, slots[s], c)
        return rcopy(at, at, cs, cr.at[j], {"core": co})

    def c_recv(j):
        at = G.at[j, :, :, co]
        return rcopy(at, at, cs, cr.at[j], {"core": co})

    top, low = pl.ds(0, 512), pl.ds(512, 512)
    wspec = (
        (W.at[0, top], W.at[1, top], {"y": yp}),
        (W.at[0, low], W.at[2, low], {"y": ym}),
        (W.at[0, low], W.at[1, low], {"y": yp}),
        (W.at[0, top], W.at[2, top], {"y": ym}),
        (W.at[1, top], W.at[3, top], {"y": yp}),
        (W.at[2, low], W.at[3, low], {"y": ym}),
    )

    def w_send(n):
        src, dst, dev = wspec[n]
        return rcopy(src, dst, ws, wr.at[n], dev)

    up, dn = pl.ds(0, 256), pl.ds(256, 256)
    rspec = (
        (S.at[0, up], RH.at[0], {"y": yp}),
        (S.at[0, dn], RH.at[1], {"y": ym}),
        (S.at[1, :, top], RY.at[0, :, top], {"y": yp}),
        (S.at[1, :, low], RY.at[0, :, low], {"y": yp}),
        (S.at[2, :, top], RY.at[1, :, top], {"y": ym}),
        (S.at[2, :, low], RY.at[1, :, low], {"y": ym}),
    )

    def r_send(n):
        src, dst, dev = rspec[n]
        return rcopy(src, dst, rs, rr.at[n], dev)

    def a_send(h):
        at = pl.ds(h * HD, HD)
        return rcopy(AT.at[at], AT2.at[at], ats, atr.at[h], {"xlo": xo})

    def p_send(h):
        return rcopy(PS.at[h], PR.at[h], ps, pr.at[h], {"xlo": xo})

    def add_into(dst, rows, srcs):
        @pl.loop(0, rows // 64)
        def _(n):
            at = pl.ds(pl.multiple_of(n * 64, 64), 64)
            total = dst[at].astype(F32)
            for src in srcs:
                total = total + src[at].astype(F32)
            dst[at] = total.astype(BF)

    def columns_of(j, at):
        return G[j, :, :, :, :, at].reshape(1024, 512)

    def tile(n, first=0):
        return pl.ds(pl.multiple_of(n * 512 + first, 512), 512)

    def weight_part(rows):
        @pl.loop(0, 2)
        def _(n):
            at = tile(n)
            total = dot(AT[rows], columns_of(0, at)) + dot(AT2[rows], columns_of(1, at))
            S[0, rows, at] = total.astype(BF)

    def pair_part(q):
        @pl.loop(0, 2)
        def _(n):
            at = tile(n)
            WT[q - 1, :, at] = dot(AT2[...], columns_of(pair_chunk[q], at))

    def own_part(q, j, shift, first, count):
        @pl.loop(0, count // 512)
        def _(n):
            at = tile(n, first)
            total = WT[q - 1, :, at] + dot(AT[...], columns_of(j, tile(n, shift)))
            S[q, :, at] = total.astype(BF)

    def att_part(acc, j, slot):
        @pl.loop(0, 2)
        def _(a):
            at = pl.ds(pl.multiple_of(a * 512, 512), 512)
            rows = G[j, a].reshape(512, 1024)
            if isinstance(slot, int):
                acc[at] += dot(rows, W[slot])
            else:
                acc[at] += dot(rows[:, :512], W[2, slot]) + dot(rows[:, 512:], W[1, slot])

    def w_start(*which):
        for n in which:
            w_send(n).start()

    def w_wait(*which):
        for n in which:
            w_send(n).wait_recv()

    first = G.at[pl.ds(0, 4), 0, 0, 0]
    pltpu.make_async_copy(first, first, ls.at[0]).wait()
    wcp.wait()
    for d in range(2):
        u_send(0, d, 0).start()
    w_start(0, 1, 2, 3)
    x_send(0).start()
    for d in range(2):
        u_send(5, d, 0).start()
    for q in range(4):
        for other in range(2):
            e_send(q, other).start()
    pltpu.make_async_copy(GA, GA, ls.at[2]).wait()
    for h in range(4):
        AT[h * HD : (h + 1) * HD] = GA[h].T
    pltpu.make_async_copy(Q, Q, ls.at[3]).wait()
    for cp in others:
        cp.wait()
    KT[...] = K[...].T
    ACC[...] = jnp.zeros_like(ACC)
    PG[...] = jnp.zeros_like(PG)

    def prob_part(h):
        stat = ST[pl.ds(h, 1)]
        for r in range(4):
            lo = r * 256
            n = 1024 - lo
            scores = dot(K[lo : lo + 256], Q[h, lo:], NT) * scale
            keys_at = lax.broadcasted_iota(jnp.int32, (256, n), 0)
            query_at = lax.broadcasted_iota(jnp.int32, (256, n), 1)
            value = jnp.exp(scores - stat[:, lo:])
            PT[r][h] = jnp.where(keys_at <= query_at, value, 0.0).astype(BF)

    def u_own(j):
        for d in range(2):
            u_send(j, d, 0).start()

    def pump(j):
        if j in pair_chunk:
            e_recv(j - 1, 1).wait_recv()
        else:
            x_recv(j).wait_recv()
        u_send(j, 0, 1).start()
        u_send(j, 1, 1).start()
        c_send(j, 0).start()

    def feed(q):
        e_recv(q, 0).wait_recv()
        u_own(q + 1)

    def relay(j):
        for d in range(2):
            u_recv(j, d).wait_recv()
            z_send(j, d).start()
        c_send(j, 1).start()
        c_send(j, 2).start()

    def land(j):
        z_recv(j).wait_recv()
        c_send(j, 3).start()

    def take(j):
        c_recv(j).wait_recv()

    def a_wait(*which):
        for h in which:
            a_send(h).wait_recv()

    for h in range(4):
        a_send(h).start()
    for j in (5, 6, 7):
        x_send(j).start()
    pump(0)
    feed(0)
    pump(1)
    prob_part(0)
    relay(0)
    feed(1)
    pump(2)
    w_wait(0, 1)
    w_start(4, 5)
    prob_part(1)
    relay(1)
    feed(2)
    pump(3)
    prob_part(2)
    land(0)
    prob_part(3)
    relay(2)
    feed(3)
    pump(4)
    land(1)
    take(0)
    take(1)
    a_wait(0, 1)
    weight_part(up)
    r_send(0).start()
    relay(3)
    w_wait(2, 3, 4, 5)
    att_part(ACC, 0, 3)
    land(2)
    att_part(PG, 1, 3)
    take(2)
    a_wait(2, 3)
    weight_part(dn)
    r_send(1).start()
    relay(4)
    pump(5)
    u_own(6)
    att_part(PG, 2, 2)
    land(3)
    take(3)
    att_part(PG, 3, 1)
    land(4)
    relay(5)
    pump(6)
    u_own(7)
    pump(7)
    take(4)
    att_part(PG, 4, 0)
    for h in range(4):
        PS[h] = PG[:, h * HD : (h + 1) * HD].astype(BF)
        p_send(h).start()
    pair_part(1)
    land(5)
    pair_part(2)
    take(5)
    own_part(1, 5, 0, 0, 512)
    r_send(0).wait_recv()
    add_into(S.at[1, up, top], 256, [RH.at[0, :, top]])
    r_send(2).start()
    own_part(2, 5, 512, 0, 512)
    r_send(1).wait_recv()
    add_into(S.at[2, dn, top], 256, [RH.at[1, :, top]])
    r_send(4).start()
    relay(6)
    pair_part(3)
    att_part(ACC, 5, top)
    relay(7)
    land(6)
    take(6)
    own_part(1, 6, 0, 512, 512)
    add_into(S.at[1, up, low], 256, [RH.at[0, :, low]])
    r_send(3).start()
    own_part(2, 6, 512, 512, 512)
    add_into(S.at[2, dn, low], 256, [RH.at[1, :, low]])
    r_send(5).start()
    land(7)
    att_part(ACC, 6, low)
    take(7)
    att_part(ACC, 7, 0)

    zh = lax.rem(z, 2)

    def kv_first(r):
        return rcopy(KB.at[r, :, :, 1 - c], KR1.at[r], ks.at[0], kr.at[0, r], {"core": co})

    def kv_second(r):
        return rcopy(KB2.at[r, 1 - zh], KR2.at[r], ks.at[1], kr.at[1, r], {"z": zpair})

    def kv_middle(r):
        kv_first(r).wait_recv()
        for n in range(2):
            for half in range(2):
                total = KF[r, n, half, c] + KR1[r, n, half].astype(F32)
                KS[r, n, half] = total
                KB2[r, half, n] = total.astype(BF)
        kv_second(r).start()

    for h in range(4):
        cols = slice(h * HD, (h + 1) * HD)
        p_send(h).wait_recv()
        part = (ACC[:, cols] + PR[h].astype(F32)).astype(BF)
        GA[h] = part
        offset = jnp.sum(part.T.astype(F32) * AT[cols].astype(F32), axis=0, keepdims=True)
        for r in range(4):
            lo = r * 256
            mine = slice(lo, lo + 256)
            attention = PT[r][h]
            gb = GA[h, lo:]
            dv = dot(attention, gb)
            grad_att = dot(V[mine], gb, NT)
            grad_scores = (attention.astype(F32) * (grad_att - offset[:, lo:])).astype(BF)
            dk = dot(grad_scores, Q[h, lo:])
            dq = dot(KT[:, mine], grad_scores)
            if r > 0:
                dq = dq + DQ[:, lo:]
            DQ[:, lo:] = dq
            dq_out[mine, cols] = (dq[:, :256] * scale).T.astype(BF)
            if h > 0:
                dv = dv + DV[r]
                dk = dk + DK[r]
            if h < 3:
                DV[r] = dv
                DK[r] = dk
                continue
            for n, full in enumerate(((dk * scale).T, dv.T)):
                for half in range(2):
                    for core in range(2):
                        at = half * 64 + core * 32
                        KF[r, n, half, core] = full[at : at + 32]
                        KB[r, n, half, core] = full[at : at + 32].astype(BF)
            kv_first(r).start()
            if r > 0:
                kv_middle(r - 1)
    kv_middle(3)
    for half in range(2):
        at = tile(half)
        WT[2, :, at] += dot(AT[...], columns_of(7, at))
    for half in range(2):
        r_send(2 + half).wait_recv()
        r_send(4 + half).wait_recv()
        at = tile(half)
        total = WT[2, :, at] + RY[0, :, at].astype(F32) + RY[1, :, at].astype(F32)
        wg_out[at] = total.T.astype(BF)

    for r in range(4):
        kv_second(r).wait_recv()
        for n in range(2):
            total = KS[r, n, zh] + KR2[r, n].astype(F32)
            (dk_out, dv_out)[n][:, r * 256 : r * 256 + 256] = total.astype(BF)

    for ref, sem in (
        (G.at[:, 0, 0, 0], es),
        (first, xs),
        (G.at[pl.ds(0, 2)], us),
        (G.at[0], zs),
        (G.at[pl.ds(0, 4)], cs),
        (W.at[pl.ds(0, 3)], ws),
        (S, rs),
        (AT, ats),
        (PS, ps),
        (KR1, ks.at[0]),
        (KR2, ks.at[1]),
    ):
        rcopy(ref, ref, sem, sem, {"core": co}).wait_send()


def finish(*refs):
    sems = refs[8]
    copies = [pltpu.make_async_copy(refs[n], refs[4 + n], sems.at[n]) for n in range(4)]
    for cp in copies:
        cp.start()
    for cp in copies:
        cp.wait()


def per_device(grad_out, out_weight, query, keys, values, attended, stats):
    any_spec = pl.BlockSpec(memory_space=pl.ANY)
    vmem = pl.BlockSpec(memory_space=pltpu.VMEM)
    V_ = pltpu.VMEM
    dma = pltpu.SemaphoreType.DMA
    scratch = [
        V_((8, 2, 4, 2, 64, 1024), BF),
        V_((4, 1024, 512), BF),
        V_((3, 512, 1024), BF),
        V_((2, 256, 1024), BF),
        V_((2, 512, 1024), BF),
        V_((512, 1024), BF),
        V_((512, 1024), BF),
        V_((3, 512, 1024), F32),
        V_((1024, 512), F32),
        V_((1024, 512), F32),
        V_((4, 1024, HD), BF),
        V_((4, 1024, HD), BF),
        V_((4, 1024, HD), BF),
        V_((4, 1024, HD), BF),
        V_((1024, HD), BF),
        V_((1024, HD), BF),
        V_((HD, 1024), BF),
        V_((4, 1024), F32),
        V_((4, 256, 1024), BF),
        V_((4, 256, 768), BF),
        V_((4, 256, 512), BF),
        V_((4, 256, 256), BF),
        V_((HD, 1024), F32),
        V_((4, 256, HD), F32),
        V_((4, 256, HD), F32),
        V_((4, 2, 2, 2, 32, 256), F32),
        V_((4, 2, 2, 2, 32, 256), BF),
        V_((4, 2, 2, 32, 256), F32),
        V_((4, 2, 2, 32, 256), BF),
        V_((4, 2, 2, 32, 256), BF),
        V_((4, 2, 32, 256), BF),
        dma, dma((8,)),
        dma, dma((4, 2)),
        dma, dma((8, 2)),
        dma, dma((8,)),
        dma, dma((8,)),
        dma, dma((6,)),
        dma, dma((6,)),
        dma, dma((4,)),
        dma, dma((4,)),
        dma((2,)), dma((2, 4)),
        dma((7,)),
    ]
    dq, dk, dv, wg = pl.pallas_call(
        kernel,
        out_shape=(
            V_((1024, 512), BF),
            V_((32, 1024), BF),
            V_((32, 1024), BF),
            V_((1024, 512), BF),
        ),
        in_specs=[any_spec] * 7,
        out_specs=(vmem,) * 4,
        scratch_shapes=scratch,
        compiler_params=pltpu.CompilerParams(
            collective_id=0, has_side_effects=True, vmem_limit_bytes=58_700_000
        ),
    )(grad_out, out_weight, query, keys, values, attended, stats)
    results = (dq, dk, dv, wg)
    dq, dk, dv, wg = pl.pallas_call(
        finish,
        out_shape=tuple(jax.ShapeDtypeStruct(r.shape, r.dtype) for r in results),
        in_specs=[any_spec] * 4,
        out_specs=(any_spec,) * 4,
        scratch_shapes=[dma((4,))],
        compiler_params=pltpu.CompilerParams(vmem_limit_bytes=1 << 20),
    )(*results)
    return (dq, dk.T, dv.T, wg)


def solution(mesh):
    torus = Mesh(mesh.devices.reshape(4, 2, 2, 4, 2), AXES)
    dp, tp = ("y", "xlo"), ("xhi", "z", "core")
    in_specs = (
        P(dp + tp, None),
        P(dp, tp),
        P(dp, tp),
        P(dp, None),
        P(dp, None),
        P(dp, tp),
        P(tp, dp),
    )
    out_specs = (P(dp, tp), P(dp, tp), P(dp, tp), P(dp, tp))
    return jax.shard_map(
        per_device, mesh=torus, in_specs=in_specs, out_specs=out_specs, check_vma=False
    )
```
